32 devices in a mesh: grp: 4 (over y, x), sub: 8 (over z, core).
Axes of the slice: x: 2, y: 2, z: 4, core: 2. Of those that a mesh axis runs over, the one named last changes fastest.
Arguments:
- reg_disp: float32 [4, 8, 3, 384], P('grp', 'sub'), may hold values from -6 to 6
- reg_vel: float32 [4, 8, 3, 384], P('grp', 'sub'), may hold values from -0.6 to 0.6
- site_disp: float32 [4, 8, 3, 1536], P('grp', 'sub'), may hold values from -6 to 6
- site_vel: float32 [4, 8, 3, 1536], P('grp', 'sub'), may hold values from -0.6 to 0.6
- reg_nodes: int32 [4, 8, 10, 256], P('grp', 'sub'), may hold values from 0 to 383
- site_nodes: int32 [4, 8, 35, 128], P('grp', 'sub'), may hold values from 0 to 1535
- reg_coefs: float32 [4, 8, 3, 3, 4, 256], P('grp', 'sub'), may hold values from -1.5 to 6, as said below
- site_coefs: float32 [4, 8, 3, 3, 24, 128], P('grp', 'sub'), may hold values from -1.5 to 6, as said below
- reg_table: float32 [12, 10], replicated, may hold values from -2 to 2
- site_table: float32 [72, 35], replicated, may hold values from -1 to 1
- reg_minv: float32 [4, 8, 384], P('grp', 'sub'), may hold values from 0.003 to 0.015
- site_minv: float32 [4, 8, 1536], P('grp', 'sub'), may hold values from 0.003 to 0.015
- reg_send: int32 [4, 8, 2, 128], P('grp', 'sub'), may hold values from 0 to 383
- reg_recv: int32 [4, 8, 2, 128], P('grp', 'sub'), may hold values from 0 to 383
- site_send: int32 [4, 8, 2, 128], P('grp', 'sub'), may hold values from 0 to 1535
- site_recv: int32 [4, 8, 2, 128], P('grp', 'sub'), may hold values from 0 to 1535
- slot_fill: int32 [4, 8, 4], P('grp', 'sub'), may hold values from 1 to 128, 384 in all within a row
- layer_src: int32 [4, 8, 128], P('grp', 'sub'), may hold values from 0 to 383
- layer_fill: int32 [4, 8], P('grp', 'sub'), may hold values from 64 to 128, as said below
- layer_dst: int32 [4, 8, 3, 128], P('grp', 'sub'), may hold values from 0 to 1535
- layer_stiff: float32 [4, 8, 3, 128], P('grp', 'sub'), may hold values from 0.5 to 2
Outputs:
- reg_final: float32 [4, 8, 3, 384], P('grp', 'sub')
- site_final: float32 [4, 8, 3, 1536], P('grp', 'sub')
The draws below stay inside these ranges and needn't reach their ends.
Inputs may be any that keep to these rules, and one draw needn't show every extreme that they name: `slot_fill`: per partition the four entries count live slots toward the lower and higher neighbour, regional then site; they sum to 384. `layer_fill`: partition index 0 of every group fills all 128 slots. `reg_coefs`: each 3 x 3 tensor over the first two dimensions is symmetric positive definite. `site_coefs`: each 3 x 3 tensor over the first two dimensions is symmetric positive definite.
All inputs are finite; a program needn't handle non-finite values.
Results may differ from the reference program's by a relative error of at most 0.0003.
Values sent between devices are 32-bit elements; how exact they have to be, the bound alone decides.
A program may use at most 64 MiB of HBM per device.

```python
import math
import jax
import jax.numpy as jnp
import numpy as np
from jax import lax

PR = 10
QR = 4
PS = 35
QS = 24
STEPS = 8
ES = 128
SLOTS = 128
DRM = 128
ER = 256
NR = 384
NS = 1536
N_GRP = 4
N_SUB = 8


def tensor_draw(key, quad_count, elem_count):
    first_key, second_key = jax.random.split(key)
    shape_diag = (N_GRP, N_SUB, 3, quad_count, elem_count)
    diagonal = jnp.exp(jax.random.uniform(first_key, shape_diag, jnp.float32, math.log(0.5), math.log(4.0)))
    off_diag = jax.random.uniform(second_key, (N_GRP, N_SUB, 3, 3, quad_count, elem_count), jnp.float32, -0.25, 0.25)
    off_diag = 0.5 * (off_diag + jnp.swapaxes(off_diag, 2, 3))
    identity = jnp.eye(3, dtype=jnp.float32)[:, :, None, None]
    off_diag = off_diag * (1.0 - identity)
    root_scale = jnp.sqrt(diagonal)
    return root_scale[:, :, :, None] * root_scale[:, :, None, :] * (identity + off_diag)


def draw_reg_coefs(key, part):
    return tensor_draw(jax.random.fold_in(key, 11), QR, ER)


def draw_site_coefs(key, part):
    return tensor_draw(jax.random.fold_in(key, 23), QS, ES)


def draw_layer_fill(key, part):
    counts = jax.random.randint(jax.random.fold_in(key, 37), (N_GRP, N_SUB), DRM // 2, DRM + 1, dtype=jnp.int32)
    return counts.at[:, 0].set(DRM)


def touch_ends(array, rng, low, high):
    place = [jax.random.randint(jax.random.fold_in(rng, axis), (), 0, length) for axis, length in enumerate(array.shape)]
    main_axis = array.shape.index(max(array.shape))
    next_to = place[:main_axis] + [(place[main_axis] + 1) % array.shape[main_axis]] + place[main_axis + 1:]
    return array.at[tuple(place)].set(low).at[tuple(next_to)].set(high)


def block_scale(key, shape, shards, low, high):
    def one(dim, blocks):
        heights = jax.random.uniform(jax.random.fold_in(jax.random.fold_in(key, 6), dim), (blocks,), jnp.float32, low / len(shards), high / len(shards))
        return jnp.repeat(jnp.exp(heights), shape[dim] // blocks).reshape((-1,) + (1,) * (len(shape) - dim - 1))

    loudness = one(*shards[0])
    for cut in shards[1:]:
        loudness = loudness * one(*cut)
    return loudness


def length_profile(count, total, bound, slope):
    weights = [(1 << 20) // math.isqrt(grade ** slope) + 1 for grade in range(2, count + 1)]
    surplus, given = total - bound - (count - 1), [1] * (count - 1)
    while surplus > 0:
        free = [i for i in range(count - 1) if given[i] < bound]
        whole, budget = sum([weights[i] for i in free]), surplus
        for i in free:
            more = min(bound - given[i], max(1, budget * weights[i] // whole), surplus)
            given[i] = given[i] + more
            surplus = surplus - more
    return np.array([bound] + given)


def ragged_sizes(stream_key, amount, total, limit, lean):
    if amount == 2:
        one = jax.random.randint(stream_key, (), max(1, total - limit), min(limit, total - 1) + 1)
        return jnp.stack([one, total - one])
    tallies = jnp.asarray(length_profile(amount, total, limit, lean), jnp.int32)
    couples = (amount - 1) // 2
    donor, sink = tallies[1:1 + 2 * couples:2], tallies[2:2 + 2 * couples:2]
    margin = jnp.minimum(donor - 1, limit - sink)
    passed = jax.random.randint(jax.random.fold_in(stream_key, 1), (couples,), 0, 1 << 20) % (margin + 1)
    tallies = tallies.at[1:1 + 2 * couples:2].set(donor - passed).at[2:2 + 2 * couples:2].set(sink + passed)
    return tallies[jax.random.permutation(jax.random.fold_in(stream_key, 2), amount)]


def scatter_about(rng, shape, spread, bound, shards=(), held_as=jnp.bfloat16):
    entries = jax.random.normal(rng, shape, jnp.float32) * spread
    if len(shards) > 0:
        entries = block_scale(rng, shape, shards, -0.22, 0.18) * entries
    return jnp.clip(entries, min=-bound, max=bound).astype(held_as)


def setup_inputs(seed: int = 0) -> dict:
    key_list = jax.random.split(jax.random.key(seed), 22)
    reg_disp = scatter_about(key_list[0], (N_GRP, N_SUB, 3, NR), 1.0, 6.0, ((0, 4), (1, 8)), jnp.float32)
    reg_vel = scatter_about(key_list[1], (N_GRP, N_SUB, 3, NR), 0.1, 0.6, ((0, 4), (1, 8)), jnp.float32)
    site_disp = scatter_about(key_list[2], (N_GRP, N_SUB, 3, NS), 1.0, 6.0, ((0, 4), (1, 8)), jnp.float32)
    site_vel = scatter_about(key_list[3], (N_GRP, N_SUB, 3, NS), 0.1, 0.6, ((0, 4), (1, 8)), jnp.float32)
    reg_nodes = touch_ends(jax.random.randint(key_list[4], (N_GRP, N_SUB, PR, ER), 0, NR), jax.random.fold_in(key_list[4], 1), 0, NR - 1).astype(jnp.int32)
    site_nodes = touch_ends(jax.random.randint(key_list[5], (N_GRP, N_SUB, PS, ES), 0, NS), jax.random.fold_in(key_list[5], 1), 0, NS - 1).astype(jnp.int32)
    reg_coefs = draw_reg_coefs(jax.random.fold_in(key_list[21], 71), 0)
    site_coefs = draw_site_coefs(jax.random.fold_in(key_list[21], 71), 0)
    reg_table = scatter_about(key_list[8], (3 * QR, PR), PR ** -0.5, 2.0, (), jnp.float32)
    site_table = scatter_about(key_list[9], (3 * QS, PS), PS ** -0.5, 1.0, (), jnp.float32)
    reg_minv = jnp.clip(jnp.exp(math.log(0.015) - 1.60943788 * jax.random.uniform(key_list[10], (N_GRP, N_SUB, NR), jnp.float32) ** block_scale(key_list[10], (N_GRP, N_SUB, NR), ((0, 4), (1, 8)), -0.2, 0.2)), 0.003, 0.015)
    site_minv = jnp.clip(jnp.exp(math.log(0.015) - 1.60943788 * jax.random.uniform(key_list[11], (N_GRP, N_SUB, NS), jnp.float32) ** block_scale(key_list[11], (N_GRP, N_SUB, NS), ((0, 4), (1, 8)), -0.2, 0.2)), 0.003, 0.015)
    reg_send = touch_ends(jax.random.randint(key_list[12], (N_GRP, N_SUB, 2, SLOTS), 0, NR), jax.random.fold_in(key_list[12], 1), 0, NR - 1).astype(jnp.int32)
    reg_recv = touch_ends(jax.random.randint(key_list[13], (N_GRP, N_SUB, 2, SLOTS), 0, NR), jax.random.fold_in(key_list[13], 1), 0, NR - 1).astype(jnp.int32)
    site_send = touch_ends(jax.random.randint(key_list[14], (N_GRP, N_SUB, 2, SLOTS), 0, NS), jax.random.fold_in(key_list[14], 1), 0, NS - 1).astype(jnp.int32)
    site_recv = touch_ends(jax.random.randint(key_list[15], (N_GRP, N_SUB, 2, SLOTS), 0, NS), jax.random.fold_in(key_list[15], 1), 0, NS - 1).astype(jnp.int32)
    slot_fill = jax.vmap(lambda own: ragged_sizes(own, 4, 3 * SLOTS, SLOTS, 0))(jax.random.split(key_list[16], N_GRP * N_SUB)).reshape((N_GRP, N_SUB, 4)).astype(jnp.int32)
    layer_src = touch_ends(jax.random.randint(key_list[17], (N_GRP, N_SUB, DRM), 0, NR), jax.random.fold_in(key_list[17], 1), 0, NR - 1).astype(jnp.int32)
    layer_fill = draw_layer_fill(jax.random.fold_in(key_list[21], 71), 0)
    layer_dst = touch_ends(jax.random.randint(key_list[19], (N_GRP, N_SUB, 3, DRM), 0, NS), jax.random.fold_in(key_list[19], 1), 0, NS - 1).astype(jnp.int32)
    layer_stiff = jnp.clip(jnp.exp(math.log(2.0) - 1.3862944 * jax.random.uniform(key_list[20], (N_GRP, N_SUB, 3, DRM), jnp.float32) ** block_scale(key_list[20], (N_GRP, N_SUB, 3, DRM), ((0, 4), (1, 8)), -0.2, 0.2)), 0.5, 2.0)
    return {"reg_disp": reg_disp, "reg_vel": reg_vel, "site_disp": site_disp, "site_vel": site_vel, "reg_nodes": reg_nodes, "site_nodes": site_nodes, "reg_coefs": reg_coefs, "site_coefs": site_coefs, "reg_table": reg_table, "site_table": site_table, "reg_minv": reg_minv, "site_minv": site_minv, "reg_send": reg_send, "reg_recv": reg_recv, "site_send": site_send, "site_recv": site_recv, "slot_fill": slot_fill, "layer_src": layer_src, "layer_fill": layer_fill, "layer_dst": layer_dst, "layer_stiff": layer_stiff}


PRECISE = lax.Precision.HIGHEST


def stiff_force(displaced, element_nodes, coef_block, deriv_table):
    quad_count = coef_block.shape[2]
    node_count = element_nodes.shape[0]
    elem_count = element_nodes.shape[1]
    flat_nodes = element_nodes.reshape(-1)
    gathered = jnp.take(displaced, flat_nodes, axis=1).reshape(3, node_count, elem_count)
    gradient = jnp.einsum("kp,cpe->cke", deriv_table, gathered, precision=PRECISE)
    pieces = [gradient[:, b * quad_count:(b + 1) * quad_count] for b in range(3)]
    flux_rows = [coef_block[a, 0][None] * pieces[0] + coef_block[a, 1][None] * pieces[1] + coef_block[a, 2][None] * pieces[2] for a in range(3)]
    flux_terms = jnp.concatenate(flux_rows, axis=1)
    element_terms = jnp.einsum("kp,cke->cpe", deriv_table, flux_terms, precision=PRECISE)
    return -jnp.zeros_like(displaced).at[:, flat_nodes].add(element_terms.reshape(3, -1))


def pack_slots(forces, send_map, fill_pair):
    picked = jnp.take(forces, send_map, axis=1)
    live_slots = jnp.arange(send_map.shape[1], dtype=jnp.int32)[None, :] < fill_pair[:, None]
    return jnp.where(live_slots[:, None, :], jnp.transpose(picked, (1, 0, 2)), 0.0)


def take_slots(forces, recv_map, from_lower, from_upper):
    return forces.at[:, recv_map[0]].add(from_lower).at[:, recv_map[1]].add(from_upper)


def pack_layer(displaced, layer_src, layer_fill):
    picked = jnp.take(displaced, layer_src, axis=1)
    live_slots = jnp.arange(layer_src.shape[0], dtype=jnp.int32) < layer_fill
    return jnp.where(live_slots[None, :], picked, 0.0)


def add_layer(forces, layer_dst, layer_stiff, layer_block):
    for source in range(3):
        forces = forces.at[:, layer_dst[source]].add(layer_stiff[source][None, :] * layer_block[source])
    return forces


def neighbour_terms(send_rows, group_rows):
    shaped = send_rows.reshape((group_rows, N_SUB) + send_rows.shape[1:])
    blank_rows = jnp.zeros_like(shaped[:, :1, 0])
    from_lower = jnp.concatenate([blank_rows, shaped[:, :-1, 1]], axis=1)
    from_upper = jnp.concatenate([shaped[:, 1:, 0], blank_rows], axis=1)
    width = send_rows.shape[-1]
    return from_lower.reshape(-1, 3, width), from_upper.reshape(-1, 3, width)


def reference(reg_disp, reg_vel, site_disp, site_vel, reg_nodes, site_nodes, reg_coefs, site_coefs, reg_table, site_table, reg_minv, site_minv, reg_send, reg_recv, site_send, site_recv, slot_fill, layer_src, layer_fill, layer_dst, layer_stiff):
    site_groups = N_GRP // 4
    reg_groups = 3 * site_groups

    def regional(stacked):
        return stacked[:reg_groups].reshape((reg_groups * N_SUB,) + stacked.shape[2:])

    def sitewise(stacked):
        return stacked[reg_groups:].reshape((site_groups * N_SUB,) + stacked.shape[2:])

    reg_now = regional(reg_disp)
    reg_prev = reg_now - regional(reg_vel)
    r_nodes, r_coefs, r_minv = regional(reg_nodes), regional(reg_coefs), regional(reg_minv)
    r_send, r_recv, r_fill = regional(reg_send), regional(reg_recv), regional(slot_fill)[:, 0:2]
    r_src, r_layer_fill = regional(layer_src), regional(layer_fill)
    layers = []
    for step_no in range(STEPS):
        forces = lax.map(lambda device_items: stiff_force(device_items[0], device_items[1], device_items[2], reg_table), (reg_now, r_nodes, r_coefs))
        send_rows = jax.vmap(pack_slots)(forces, r_send, r_fill)
        from_lower, from_upper = neighbour_terms(send_rows, reg_groups)
        forces = jax.vmap(take_slots)(forces, r_recv, from_lower, from_upper)
        reg_next = 2.0 * reg_now - reg_prev + r_minv[:, None, :] * forces
        reg_prev, reg_now = reg_now, reg_next
        layers.append(jax.vmap(pack_layer)(reg_now, r_src, r_layer_fill))

    site_now = sitewise(site_disp)
    site_prev = site_now - sitewise(site_vel)
    s_nodes, s_coefs, s_minv = sitewise(site_nodes), sitewise(site_coefs), sitewise(site_minv)
    s_send, s_recv, s_fill = sitewise(site_send), sitewise(site_recv), sitewise(slot_fill)[:, 2:4]
    s_dst, s_stiff = sitewise(layer_dst), sitewise(layer_stiff)
    for step_no in range(STEPS):
        forces = lax.map(lambda device_items: stiff_force(device_items[0], device_items[1], device_items[2], site_table), (site_now, s_nodes, s_coefs))
        send_rows = jax.vmap(pack_slots)(forces, s_send, s_fill)
        from_lower, from_upper = neighbour_terms(send_rows, site_groups)
        forces = jax.vmap(take_slots)(forces, s_recv, from_lower, from_upper)
        layer_block = layers[step_no].reshape(3, site_groups, N_SUB, 3, -1)
        layer_block = jnp.transpose(layer_block, (1, 2, 0, 3, 4)).reshape(site_groups * N_SUB, 3, 3, -1)
        forces = jax.vmap(add_layer)(forces, s_dst, s_stiff, layer_block)
        site_next = 2.0 * site_now - site_prev + s_minv[:, None, :] * forces
        site_prev, site_now = site_now, site_next

    reg_final = jnp.concatenate([reg_now.reshape((reg_groups, N_SUB) + reg_now.shape[1:]),
                                 jnp.zeros((site_groups, N_SUB) + reg_now.shape[1:], jnp.float32)], axis=0)
    site_final = jnp.concatenate([jnp.zeros((reg_groups, N_SUB) + site_now.shape[1:], jnp.float32),
                                  site_now.reshape((site_groups, N_SUB) + site_now.shape[1:])], axis=0)
    return reg_final, site_final
```

```python
import functools

import jax
import jax.numpy as jnp
from jax import lax
from jax.experimental import pallas as pl
from jax.experimental.pallas import tpu as pltpu
from jax.sharding import PartitionSpec as P

STEPS = 8
LANES = 128
MESH = pl.DeviceIdType.MESH
F32 = jnp.float32
BF16 = jnp.bfloat16


def up(size, unit):
    return -(-size // unit) * unit


def lane_gather(block, index):
    numbers = lax.GatherDimensionNumbers(
        offset_dims=(),
        collapsed_slice_dims=(1,),
        start_index_map=(1,),
        operand_batching_dims=(0,),
        start_indices_batching_dims=(0,),
    )
    return lax.gather(
        block,
        index[..., None],
        numbers,
        slice_sizes=(1, 1),
        mode=lax.GatherScatterMode.PROMISE_IN_BOUNDS,
    )


def split(value):
    high = value.astype(BF16)
    low = (value - high.astype(F32)).astype(BF16)
    return high, low


def dot(left, right):
    return jnp.dot(left, right, preferred_element_type=F32)


def sizes(nodes_shape, coefs_shape, disp_shape):
    p, _, e = nodes_shape
    q = coefs_shape[-2]
    count = disp_shape[-1]
    width = LANES
    h = -(-count // width)
    qp = up(q, 8)
    return dict(
        p=p, e=e, q=q, count=count, width=width, shift=width.bit_length() - 1, h=h, hp=up(h, 8), qp=qp,
        p8=up(p, 8), pp=up(p, 16), kp=up(3 * qp, 16),
    )


def role_scratch(d, slot_rows, slots):
    return dict(
        lane=pltpu.VMEM((d["p8"], d["e"]), jnp.int32),
        block=pltpu.VMEM((d["p8"], d["e"]), jnp.int32),
        hot=pltpu.VMEM((d["p"] * d["e"], d["width"]), BF16),
        slot_hot=pltpu.VMEM((slot_rows * slots, d["width"]), BF16),
        fe=pltpu.VMEM((2, d["pp"], 3 * d["e"]), F32),
        coef=pltpu.VMEM((9, d["qp"], d["e"]), F32),
        dd=pltpu.VMEM((d["kp"], 3 * d["pp"]), BF16),
        dt=pltpu.VMEM((d["pp"], 3 * d["kp"]), BF16),
        u=pltpu.VMEM((3 * d["hp"], d["width"]), F32),
        prev=pltpu.VMEM((3 * d["hp"], d["width"]), F32),
        minv=pltpu.VMEM((3 * d["hp"], d["width"]), F32),
        turn=pltpu.VMEM((LANES, max(d["e"], slots)), F32),
    )


def fill_onehot(d, out_ref, rows, turn):
    length = rows[0].shape[1]
    for r, row in enumerate(rows):
        turn[r : r + 1, 0:length] = (row & (d["width"] - 1)).astype(F32)
    columns = turn[:, 0:length].T
    lane = lax.broadcasted_iota(jnp.int32, (length, d["width"]), 1).astype(F32)
    for r in range(len(rows)):
        hot = jnp.where(lane == columns[:, r : r + 1], 1.0, 0.0)
        out_ref[r * length : (r + 1) * length, :] = hot.astype(BF16)


def fill_tables(d, s, table, square):
    p, q, qp, kp, pp = d["p"], d["q"], d["qp"], d["kp"], d["pp"]
    square[...] = jnp.zeros_like(square)
    turned = table.shape[0] == p
    for b in range(3):
        if turned:
            square[0:p, b * qp : b * qp + q] = table[:, b * q : (b + 1) * q]
        else:
            square[b * qp : b * qp + q, 0:p] = table[b * q : (b + 1) * q, :]

    def plain():
        high, low = split(square[0:kp, 0:pp])
        s["dd"][...] = jnp.concatenate([high.astype(F32), low.astype(F32), high.astype(F32)], axis=1).astype(BF16)

    def flipped():
        high, low = split(-square[0:pp, 0:kp])
        s["dt"][...] = jnp.concatenate([high.astype(F32), low.astype(F32), high.astype(F32)], axis=1).astype(BF16)

    first, second = (flipped, plain) if turned else (plain, flipped)
    first()
    square[...] = square[...].T
    second()


def fill_nodes(d, s, nodes, slot_rows):
    p = d["p"]
    s["lane"][...] = jnp.zeros_like(s["lane"])
    s["block"][...] = jnp.full_like(s["block"], -1)
    for r in range(p):
        s["lane"][r : r + 1, :] = nodes[r] & (LANES - 1)
        s["block"][r : r + 1, :] = nodes[r] >> 7
    s["turn"][...] = jnp.zeros_like(s["turn"])
    fill_onehot(d, s["hot"], [nodes[r] for r in range(p)], s["turn"])
    fill_onehot(d, s["slot_hot"], slot_rows, s["turn"])


def fill_state(d, s, disp, vel, minv):
    hp, width, count = d["hp"], d["width"], d["count"]
    for ref in (s["u"], s["prev"], s["minv"]):
        ref[...] = jnp.zeros_like(ref)
    for c in range(3):
        for h in range(d["h"]):
            size = min(width, count - h * width)
            at, cut = c * hp + h, slice(h * width, h * width + size)
            now = disp[c, :, cut]
            s["u"][at : at + 1, 0:size] = now
            s["prev"][at : at + 1, 0:size] = now - vel[c, :, cut]
            s["minv"][at : at + 1, 0:size] = minv[0, :, cut]


def fill_coefs(d, s, coefs):
    if d["qp"] != d["q"]:
        s["coef"][...] = jnp.zeros_like(s["coef"])
    s["coef"][:, 0 : d["q"], :] = coefs[...]


def spread(d, rows, blocks):
    lanes = rows[0].shape[1]
    mine = lax.broadcasted_iota(jnp.int32, (d["hp"], lanes), 0) == blocks
    return jnp.concatenate([jnp.where(mine, row, 0.0) for row in rows], axis=0).astype(BF16)


def spread_block(d, block, index):
    high = block.astype(BF16).astype(F32)
    low = block - high
    rows = [part[c : c + 1] for part in (high, low) for c in range(3)]
    return spread(d, rows, index >> d["shift"])


def join(d, total):
    half = 3 * d["hp"]
    return total[0:half] + total[half:]


def pick(d, field, index, live):
    hp, slots = d["hp"], index.shape[1]
    lane = jnp.broadcast_to(index & (LANES - 1), (hp, slots))
    blocks = jnp.where(live, index >> d["shift"], -1)
    mine = lax.broadcasted_iota(jnp.int32, (hp, slots), 0) == blocks
    parts = d["width"] // LANES
    which = jnp.broadcast_to((index >> 7) & (parts - 1), (hp, slots))
    out = []
    for c in range(3):
        rows = field[c * hp : (c + 1) * hp]
        got = lane_gather(rows[:, 0:LANES], lane)
        for k in range(1, parts):
            got = jnp.where(which == k, lane_gather(rows[:, k * LANES : (k + 1) * LANES], lane), got)
        out.append(jnp.sum(jnp.where(mine, got, 0.0), axis=0, keepdims=True))
    return out


def element_forces(d, s):
    p, e, qp, kp, pp, p8, hp = d["p"], d["e"], d["qp"], d["kp"], d["pp"], d["p8"], d["hp"]
    parts = d["width"] // LANES
    blocks128 = -(-d["count"] // LANES)
    tiles = e // LANES
    groups = p8 // 8
    got = {}
    for t in range(tiles):
        cut = slice(t * LANES, (t + 1) * LANES)
        for g in range(groups):
            lane = s["lane"][8 * g : 8 * g + 8, cut]
            block = s["block"][8 * g : 8 * g + 8, cut]
            bits = [(block >> k) & 1 == 1 for k in range((blocks128 - 1).bit_length())]
            for c in range(3):
                values = []
                for h in range(blocks128):
                    at, part = h // parts, h % parts
                    row = s["u"][c * hp + at : c * hp + at + 1, part * LANES : (part + 1) * LANES]
                    values.append(lane_gather(jnp.broadcast_to(row, (8, LANES)), lane))
                for bit in bits:
                    values = [
                        jnp.where(bit, values[k + 1], values[k]) if k + 1 < len(values) else values[k]
                        for k in range(0, len(values), 2)
                    ]
                got[c, t, g] = values[0]
    rows = [
        jnp.concatenate([got[c, t, g] for c in range(3) for t in range(tiles)], axis=1) for g in range(groups)
    ]
    if pp != p8:
        rows.append(jnp.zeros((pp - p8, 3 * e), F32))
    high, low = split(jnp.concatenate(rows, axis=0))
    grad = dot(s["dd"][...], jnp.concatenate([high, high, low], axis=0))
    fluxes = []
    for c in range(3):
        cut = slice(c * e, (c + 1) * e)
        pieces = [grad[b * qp : (b + 1) * qp, cut] for b in range(3)]
        rows = [
            s["coef"][3 * a] * pieces[0] + s["coef"][3 * a + 1] * pieces[1] + s["coef"][3 * a + 2] * pieces[2]
            for a in range(3)
        ]
        if kp != 3 * qp:
            rows.append(jnp.zeros((kp - 3 * qp, e), F32))
        fluxes.append(jnp.concatenate(rows, axis=0))
    high, low = split(jnp.concatenate(fluxes, axis=1))
    force = dot(s["dt"][...], jnp.concatenate([high, high, low], axis=0))
    high = force.astype(BF16).astype(F32)
    s["fe"][0] = high
    s["fe"][1] = force - high
    up_shift = parts.bit_length() - 1
    step = max(1, 2 * LANES // e)
    total = None
    for first in range(0, p, step):
        chunk = range(first, min(p, first + step))
        left = []
        for n in chunk:
            rows = [s["fe"][k, n : n + 1, c * e : (c + 1) * e] for k in range(2) for c in range(3)]
            left.append(spread(d, rows, s["block"][n : n + 1, :] >> up_shift))
        piece = dot(jnp.concatenate(left, axis=1), s["hot"][first * e : (chunk[-1] + 1) * e, :])
        total = piece if total is None else total + piece
    return join(d, total)


SCALAR = 18
REG_INPUTS = (0, 1, 4, 6, 8, 10, 12, 13, 16, 17)
SITE_INPUTS = (2, 3, 5, 7, 9, 11, 14, 15, 16, 19, 20)
NAMES = ("disp", "vel", "nodes", "coefs", "table", "minv", "send", "recv", "fill", "x", "y")


def kernel(n_grp, n_sub, rd, sd, slots, *refs):
    inputs, (reg_out, site_out), refs = refs[:21], refs[21:23], refs[23:]
    (send_ref, recv_ref, layer_send_ref, layer_recv_ref, square, halo_send, halo_recv, layer_send, layer_recv, load_sem), refs = refs[:10], refs[10:]
    layer_fill = inputs[SCALAR]
    keys = list(role_scratch(rd, 2, slots))
    rs, refs = dict(zip(keys, refs)), refs[len(keys) :]
    ss, refs = dict(zip(keys, refs)), refs[len(keys) :]
    count = len(REG_INPUTS)
    reg_in, site_in = refs[:count], refs[count:]
    sites = n_grp // 4
    regs = 3 * sites
    grp, sub = lax.axis_index("grp"), lax.axis_index("sub")
    is_site = grp >= regs
    has_low, has_high = sub > 0, sub < n_sub - 1
    source, part = grp // sites, grp % sites

    def loads(numbers, places):
        return {
            name: pltpu.make_async_copy(inputs[k], place, load_sem.at[i])
            for i, (name, k, place) in enumerate(zip(NAMES, numbers, places))
        }

    reg_loads, site_loads = loads(REG_INPUTS, reg_in), loads(SITE_INPUTS, site_in)
    first = ("nodes", "recv", "x", "table", "coefs", "disp", "vel", "minv", "send", "fill", "y")

    @pl.when(jnp.logical_not(is_site))
    def _():
        for name in first[:-1]:
            reg_loads[name].start()

    @pl.when(is_site)
    def _():
        for name in first:
            site_loads[name].start()

    barrier = pltpu.get_barrier_semaphore()

    def greet(target):
        pl.semaphore_signal(barrier, inc=1, device_id=target, device_id_type=MESH)

    @pl.when(has_low)
    def _():
        greet((grp, sub - 1))

    @pl.when(has_high)
    def _():
        greet((grp, sub + 1))

    @pl.when(is_site)
    def _():
        for m in range(3):
            greet((m * sites + part, sub))

    def meet(others):
        peers = jnp.minimum(sub, 1) + jnp.minimum(n_sub - 1 - sub, 1) + others
        pl.semaphore_wait(barrier, peers)

    def halo(n, side):
        target = sub - 1 if side == 0 else sub + 1
        return pltpu.make_async_remote_copy(
            src_ref=send_ref.at[n, side],
            dst_ref=recv_ref.at[n, 1 - side],
            send_sem=halo_send.at[n, side],
            recv_sem=halo_recv.at[n, 1 - side],
            device_id=(grp, target),
            device_id_type=MESH,
        )

    def arrival(n, side):
        target = sub - 1 if side == 0 else sub + 1
        return pltpu.make_async_remote_copy(
            src_ref=send_ref.at[n, side],
            dst_ref=recv_ref.at[n, side],
            send_sem=halo_send.at[n, side],
            recv_sem=halo_recv.at[n, side],
            device_id=(grp, target),
            device_id_type=MESH,
        )

    def layer_copy(n, m):
        return pltpu.make_async_remote_copy(
            src_ref=layer_send_ref.at[n],
            dst_ref=layer_recv_ref.at[n, m],
            send_sem=layer_send.at[n],
            recv_sem=layer_recv.at[n, m],
            device_id=(regs + part, sub),
            device_id_type=MESH,
        )

    send_ref[...] = jnp.zeros_like(send_ref)

    @pl.when(jnp.logical_not(has_low))
    def _():
        recv_ref[:, 0] = jnp.zeros((STEPS, 8, slots), F32)

    @pl.when(jnp.logical_not(has_high))
    def _():
        recv_ref[:, 1] = jnp.zeros((STEPS, 8, slots), F32)

    lane = lax.broadcasted_iota(jnp.int32, (1, slots), 1)

    def exchange_start(d, n, force, send_map, fills, first_fill):
        for side in range(2):
            fill = fills[0, :, first_fill + side : first_fill + side + 1]
            rows = pick(d, force, send_map[side : side + 1, :], lane < fill)
            for c in range(3):
                send_ref[n, side, c : c + 1, :] = rows[c]

        @pl.when(has_low)
        def _():
            halo(n, 0).start()

        @pl.when(has_high)
        def _():
            halo(n, 1).start()

    def exchange_end(d, n, recv_map, hot):
        @pl.when(has_low)
        def _():
            arrival(n, 0).wait_recv()

        @pl.when(has_high)
        def _():
            arrival(n, 1).wait_recv()

        left = [spread_block(d, recv_ref[n, side], recv_map[side : side + 1, :]) for side in range(2)]
        return join(d, dot(jnp.concatenate(left, axis=1), hot))

    def step_on(s, force):
        now = s["u"][...]
        later = 2.0 * now - s["prev"][...] + s["minv"][...] * force
        s["prev"][...] = now
        s["u"][...] = later
        return later

    def finish(d, s, out):
        width, total = d["width"], d["count"]
        for c in range(3):
            for h in range(d["h"]):
                at, size = c * d["hp"] + h, min(width, total - h * width)
                out[c, :, h * width : h * width + size] = s["u"][at : at + 1, 0:size]

    def drain():
        def body(n, carry):
            @pl.when(has_low)
            def _():
                halo(n, 0).wait_send()

            @pl.when(has_high)
            def _():
                halo(n, 1).wait_send()

            return carry

        lax.fori_loop(0, STEPS, body, 0)

    @pl.when(jnp.logical_not(is_site))
    def _():
        v = dict(zip(NAMES, reg_in))
        site_out[...] = jnp.zeros_like(site_out)
        layer_send_ref[...] = jnp.zeros_like(layer_send_ref)
        for name in ("nodes", "recv"):
            reg_loads[name].wait()
        fill_nodes(rd, rs, v["nodes"], [v["recv"][k : k + 1, :] for k in range(2)])
        for name in first[:-1]:
            if name not in ("nodes", "recv"):
                reg_loads[name].wait()
        fill_tables(rd, rs, v["table"], square)
        fill_coefs(rd, rs, v["coefs"])
        fill_state(rd, rs, v["disp"], v["vel"], v["minv"])
        meet(1)

        def body(n, carry):
            force = element_forces(rd, rs)
            exchange_start(rd, n, force, v["send"], v["fill"], 0)
            force = force + exchange_end(rd, n, v["recv"], rs["slot_hot"][...])
            later = step_on(rs, force)
            rows = pick(rd, later, v["x"][0], lane < layer_fill[...])
            for c in range(3):
                layer_send_ref[n, c : c + 1, :] = rows[c]
            layer_copy(n, source).start()
            return carry

        lax.fori_loop(0, STEPS, body, 0)
        finish(rd, rs, reg_out)
        drain()

        def last(n, carry):
            layer_copy(n, source).wait_send()
            return carry

        lax.fori_loop(0, STEPS, last, 0)

    @pl.when(is_site)
    def _():
        v = dict(zip(NAMES, site_in))
        reg_out[...] = jnp.zeros_like(reg_out)
        early = ("nodes", "recv", "x")
        for name in early:
            site_loads[name].wait()
        fill_nodes(sd, ss, v["nodes"], [v["recv"][k : k + 1, :] for k in range(2)] + [v["x"][m] for m in range(3)])
        for name in first:
            if name not in early:
                site_loads[name].wait()
        fill_tables(sd, ss, v["table"], square)
        fill_coefs(sd, ss, v["coefs"])
        fill_state(sd, ss, v["disp"], v["vel"], v["minv"])
        meet(0)

        def body(n, carry):
            force = element_forces(sd, ss)
            exchange_start(sd, n, force, v["send"], v["fill"], 2)
            for m in range(3):
                layer_copy(n, m).wait_recv()
            left = [spread_block(sd, layer_recv_ref[n, m] * v["y"][m], v["x"][m]) for m in range(3)]
            force = force + join(sd, dot(jnp.concatenate(left, axis=1), ss["slot_hot"][2 * slots :, :]))
            force = force + exchange_end(sd, n, v["recv"], ss["slot_hot"][0 : 2 * slots, :])
            step_on(ss, force)
            return carry

        lax.fori_loop(0, STEPS, body, 0)
        finish(sd, ss, site_out)
        drain()


def solution(mesh):
    n_grp, n_sub = mesh.shape["grp"], mesh.shape["sub"]

    def shards(*args):
        args = list(args)
        for k in (0, 1, 2, 3, 4, 5, 19, 20):
            rows, length = args[k].shape[2:]
            args[k] = jnp.transpose(args[k], (0, 2, 1, 3)).reshape(rows, 1, length)
        for k in (12, 13, 14, 15):
            args[k] = args[k].reshape(args[k].shape[2:])
        args[9] = args[9].T
        for k in (6, 7):
            args[k] = args[k].reshape((9,) + args[k].shape[4:])
        rd = sizes(args[4].shape, args[6].shape, args[0].shape)
        sd = sizes(args[5].shape, args[7].shape, args[2].shape)
        slots = args[12].shape[1]
        vmem = pl.BlockSpec(memory_space=pltpu.VMEM)
        hbm = pl.BlockSpec(memory_space=pltpu.HBM)
        places = [pltpu.VMEM(args[k].shape, args[k].dtype) for k in REG_INPUTS + SITE_INPUTS]
        reg_out, site_out = pl.pallas_call(
            functools.partial(kernel, n_grp, n_sub, rd, sd, slots),
            out_shape=(
                jax.ShapeDtypeStruct(args[0].shape, F32),
                jax.ShapeDtypeStruct(args[2].shape, F32),
            ),
            in_specs=[vmem if k == SCALAR else hbm for k in range(len(args))],
            out_specs=(vmem, vmem),
            scratch_shapes=[
                pltpu.VMEM((STEPS, 2, 8, slots), F32),
                pltpu.VMEM((STEPS, 2, 8, slots), F32),
                pltpu.VMEM((STEPS, 8, slots), F32),
                pltpu.VMEM((STEPS, 3, 8, slots), F32),
                pltpu.VMEM((LANES, LANES), F32),
                pltpu.SemaphoreType.DMA((STEPS, 2)),
                pltpu.SemaphoreType.DMA((STEPS, 2)),
                pltpu.SemaphoreType.DMA((STEPS,)),
                pltpu.SemaphoreType.DMA((STEPS, 3)),
                pltpu.SemaphoreType.DMA((len(SITE_INPUTS),)),
            ]
            + list(role_scratch(rd, 2, slots).values())
            + list(role_scratch(sd, 5, slots).values())
            + places,
            compiler_params=pltpu.CompilerParams(
                collective_id=0, has_side_effects=True, vmem_limit_bytes=32 * 1024 * 1024
            ),
        )(*[arg if k == SCALAR else pltpu.with_memory_space_constraint(arg, pltpu.HBM) for k, arg in enumerate(args)])
        return tuple(out.reshape(1, 1, out.shape[0], out.shape[2]) for out in (reg_out, site_out))

    cell = ("grp", "sub")
    specs = [P(*cell)] * 21
    specs[8] = specs[9] = P()
    return jax.shard_map(
        shards,
        mesh=mesh,
        in_specs=tuple(specs),
        out_specs=(P(*cell), P(*cell)),
        check_vma=False,
    )
```

```python
import functools

import jax
import jax.numpy as jnp
from jax import lax
from jax.experimental import pallas as pl
from jax.experimental.pallas import tpu as pltpu
from jax.sharding import PartitionSpec as P

STEPS = 8
ROUNDS = STEPS // 2
LANES = 128
MESH = pl.DeviceIdType.MESH
F32 = jnp.float32
BF16 = jnp.bfloat16


def up(size, unit):
    return -(-size // unit) * unit


def lane_gather(block, index):
    numbers = lax.GatherDimensionNumbers(
        offset_dims=(),
        collapsed_slice_dims=(1,),
        start_index_map=(1,),
        operand_batching_dims=(0,),
        start_indices_batching_dims=(0,),
    )
    return lax.gather(
        block,
        index[..., None],
        numbers,
        slice_sizes=(1, 1),
        mode=lax.GatherScatterMode.PROMISE_IN_BOUNDS,
    )


def split(value):
    high = value.astype(BF16)
    low = (value - high.astype(F32)).astype(BF16)
    return high, low


def dot(left, right):
    return jnp.dot(left, right, preferred_element_type=F32)


def sizes(nodes_shape, coefs_shape, disp_shape):
    p, _, e = nodes_shape
    q = coefs_shape[-2]
    count = disp_shape[-1]
    width = LANES
    h = -(-count // width)
    qp = up(q, 8)
    return dict(
        p=p, e=e, q=q, count=count, width=width, shift=width.bit_length() - 1, h=h, hp=up(h, 8), qp=qp,
        p8=up(p, 8), kw=up(9 * qp, LANES),
    )


def part_scratch(d, slot_rows, slots):
    state = (3 * d["hp"], d["width"])
    return dict(
        lane=pltpu.VMEM((d["p8"], d["e"]), jnp.int32),
        block=pltpu.VMEM((d["p8"], d["e"]), jnp.int32),
        hot=pltpu.VMEM((d["p"] * d["e"], d["width"]), BF16),
        slot_hot=pltpu.VMEM((slot_rows * slots, d["width"]), BF16),
        fe=pltpu.VMEM((2, d["p8"], 3 * d["e"]), F32),
        ve=pltpu.VMEM((3, d["p8"], d["e"]), F32),
        matrix=pltpu.VMEM((d["p"] * d["p8"], d["e"]), F32),
        u=pltpu.VMEM(state, F32),
        minv=pltpu.VMEM(state, F32),
    )


def role_scratch(d, slots):
    state = (3 * d["hp"], d["width"])
    return dict(
        wide=pltpu.VMEM((2, d["p8"], d["kw"]), F32),
        weight=pltpu.VMEM((2, up(d["p"] * d["p8"], 16), d["kw"]), BF16),
        cube=pltpu.VMEM((9 * d["qp"], d["e"]), F32),
        turn=pltpu.VMEM((LANES, max(d["e"], slots)), F32),
        prev=pltpu.VMEM(state, F32),
        w_send=pltpu.VMEM((ROUNDS,) + state, F32),
        w_recv=pltpu.VMEM((ROUNDS,) + state, F32),
    )


def fill_onehot(d, out_ref, rows, turn):
    length = rows[0].shape[1]
    for r, row in enumerate(rows):
        turn[r : r + 1, 0:length] = (row & (d["width"] - 1)).astype(F32)
    columns = turn[:, 0:length].T
    lane = lax.broadcasted_iota(jnp.int32, (length, d["width"]), 1).astype(F32)
    for r in range(len(rows)):
        hot = jnp.where(lane == columns[:, r : r + 1], 1.0, 0.0)
        out_ref[r * length : (r + 1) * length, :] = hot.astype(BF16)


def fill_tables(d, s, table, square):
    p, q, qp, p8 = d["p"], d["q"], d["qp"], d["p8"]
    wide = s["wide"]
    wide[...] = jnp.zeros_like(wide)
    if table.shape[0] != p:
        square[...] = jnp.zeros_like(square)
        square[0 : 3 * q, 0:p] = table[...]
        square[...] = square[...].T
        table = square
    for a in range(3):
        for b in range(3):
            at = (3 * a + b) * qp
            wide[0, 0:p, at : at + q] = table[0:p, a * q : (a + 1) * q]
            wide[1, 0:p, at : at + q] = table[0:p, b * q : (b + 1) * q]
    left = -wide[0]
    for first in range(0, p, 2):
        rows = range(first, min(p, first + 2))
        high, low = split(jnp.concatenate([left * wide[1, n : n + 1, :] for n in rows], axis=0))
        cut = slice(first * p8, (rows[-1] + 1) * p8)
        s["weight"][0, cut, :] = high
        s["weight"][1, cut, :] = low


def fill_nodes(d, s, nodes, slot_rows):
    p = d["p"]
    s["lane"][...] = jnp.zeros_like(s["lane"])
    s["block"][...] = jnp.full_like(s["block"], -1)
    for r in range(p):
        s["lane"][r : r + 1, :] = nodes[r] & (LANES - 1)
        s["block"][r : r + 1, :] = nodes[r] >> 7
    s["turn"][...] = jnp.zeros_like(s["turn"])
    fill_onehot(d, s["hot"], [nodes[r] for r in range(p)], s["turn"])
    fill_onehot(d, s["slot_hot"], slot_rows, s["turn"])


def fill_state(d, pairs):
    hp, width, count = d["hp"], d["width"], d["count"]
    for ref, _ in pairs:
        ref[...] = jnp.zeros_like(ref)
    for c in range(3):
        for h in range(d["h"]):
            size = min(width, count - h * width)
            at, cut = c * hp + h, slice(h * width, h * width + size)
            for ref, value in pairs:
                ref[at : at + 1, 0:size] = value(c, cut)


def fill_matrix(d, s, coefs):
    q, qp, p, p8, e, depth = d["q"], d["qp"], d["p"], d["p8"], d["e"], 9 * d["qp"]
    if qp != q:
        s["cube"][...] = jnp.zeros_like(s["cube"])
    for k in range(9):
        s["cube"][k * qp : k * qp + q, :] = coefs[k]
    high, low = split(s["cube"][...])
    both = jnp.concatenate([high, low], axis=1)
    for first in range(0, p, 2):
        cut = slice(first * p8, min(p, first + 2) * p8)
        wide = dot(s["weight"][0, cut, 0:depth], both)
        s["matrix"][cut, :] = wide[:, 0:e] + wide[:, e:] + dot(s["weight"][1, cut, 0:depth], high)


def spread(d, rows, blocks):
    lanes = rows[0].shape[1]
    mine = lax.broadcasted_iota(jnp.int32, (d["hp"], lanes), 0) == blocks
    return jnp.concatenate([jnp.where(mine, row, 0.0) for row in rows], axis=0).astype(BF16)


def spread_block(d, block, index):
    high = block.astype(BF16).astype(F32)
    low = block - high
    rows = [part[c : c + 1] for part in (high, low) for c in range(3)]
    return spread(d, rows, index >> d["shift"])


def join(d, total):
    half = 3 * d["hp"]
    return total[0:half] + total[half:]


def pick(d, field, index, live):
    hp, slots = d["hp"], index.shape[1]
    lane = jnp.broadcast_to(index & (LANES - 1), (hp, slots))
    blocks = jnp.where(live, index >> d["shift"], -1)
    mine = lax.broadcasted_iota(jnp.int32, (hp, slots), 0) == blocks
    parts = d["width"] // LANES
    which = jnp.broadcast_to((index >> 7) & (parts - 1), (hp, slots))
    out = []
    for c in range(3):
        rows = field[c * hp : (c + 1) * hp]
        got = lane_gather(rows[:, 0:LANES], lane)
        for k in range(1, parts):
            got = jnp.where(which == k, lane_gather(rows[:, k * LANES : (k + 1) * LANES], lane), got)
        out.append(jnp.sum(jnp.where(mine, got, 0.0), axis=0, keepdims=True))
    return out


def element_forces(d, s):
    p, e, p8, hp = d["p"], d["e"], d["p8"], d["hp"]
    parts = d["width"] // LANES
    blocks128 = -(-d["count"] // LANES)
    groups = p8 // 8
    for t in range(e // LANES):
        cut = slice(t * LANES, (t + 1) * LANES)
        for g in range(groups):
            lane = s["lane"][8 * g : 8 * g + 8, cut]
            block = s["block"][8 * g : 8 * g + 8, cut]
            bits = [(block >> k) & 1 == 1 for k in range((blocks128 - 1).bit_length())]
            for c in range(3):
                values = []
                for h in range(blocks128):
                    at, part = h // parts, h % parts
                    row = s["u"][c * hp + at : c * hp + at + 1, part * LANES : (part + 1) * LANES]
                    values.append(lane_gather(jnp.broadcast_to(row, (8, LANES)), lane))
                for bit in bits:
                    values = [
                        jnp.where(bit, values[k + 1], values[k]) if k + 1 < len(values) else values[k]
                        for k in range(0, len(values), 2)
                    ]
                s["ve"][c, 8 * g : 8 * g + 8, cut] = values[0]
        total = [[None] * groups for _ in range(3)]
        for n in range(p):
            rows = [s["ve"][c, n : n + 1, cut] for c in range(3)]
            for g in range(groups):
                weight = s["matrix"][n * p8 + 8 * g : n * p8 + 8 * g + 8, cut]
                for c in range(3):
                    term = weight * rows[c]
                    total[c][g] = term if n == 0 else total[c][g] + term
        for g in range(groups):
            for c in range(3):
                high = total[c][g].astype(BF16).astype(F32)
                at = slice(c * e + t * LANES, c * e + (t + 1) * LANES)
                s["fe"][0, 8 * g : 8 * g + 8, at] = high
                s["fe"][1, 8 * g : 8 * g + 8, at] = total[c][g] - high
    up_shift = parts.bit_length() - 1
    step = max(1, 2 * LANES // e)
    total = None
    for first in range(0, p, step):
        chunk = range(first, min(p, first + step))
        left = []
        for n in chunk:
            rows = [s["fe"][k, n : n + 1, c * e : (c + 1) * e] for k in range(2) for c in range(3)]
            left.append(spread(d, rows, s["block"][n : n + 1, :] >> up_shift))
        piece = dot(jnp.concatenate(left, axis=1), s["hot"][first * e : (chunk[-1] + 1) * e, :])
        total = piece if total is None else total + piece
    return join(d, total)


SCALAR = 18
REG_INPUTS = (0, 1, 4, 6, 8, 10, 12, 13, 16, 17)
SITE_INPUTS = (2, 3, 5, 7, 9, 11, 14, 15, 16, 19, 20)
NAMES = ("disp", "vel", "nodes", "coefs", "table", "minv", "send", "recv", "fill", "spot", "stiff")
REG_SHARED = ("nodes", "recv", "send", "fill", "minv", "coefs")
SITE_SHARED = ("nodes", "recv", "spot", "send", "fill", "minv", "stiff", "coefs")


def kernel(n_grp, n_sub, rd, sd, slots, keys, *refs):
    inputs, (reg_out, site_out), refs = refs[:21], refs[21:23], refs[23:]
    layer_fill = inputs[SCALAR]
    box = {}
    for group, names in keys:
        box[group], refs = dict(zip(names, refs)), refs[len(names) :]
    b = box["common"]
    sites = n_grp // 4
    regs = 3 * sites
    grp, sub = lax.axis_index("grp"), lax.axis_index("sub")
    is_site = grp >= regs
    source, part = grp // sites, grp % sites
    odd = lax.rem(sub, 2)
    cross_side, mate_side = odd, 1 - odd
    way = 2 * odd - 1
    cross, mate, beyond, behind = sub + way, sub - way, sub + 2 * way, sub - 2 * way

    def exists(place):
        return jnp.logical_and(place >= 0, place < n_sub)

    has_cross, has_mate, has_beyond, has_behind = (exists(place) for place in (cross, mate, beyond, behind))

    def count(flag):
        return jnp.where(flag, 1, 0)

    def remote(src, dst, send_sem, recv_sem, target):
        return pltpu.make_async_remote_copy(
            src_ref=src, dst_ref=dst, send_sem=send_sem, recv_sem=recv_sem, device_id=target, device_id_type=MESH
        )

    def loads(numbers, places):
        return {
            name: pltpu.make_async_copy(inputs[k], places[name], b["load_sem"].at[i])
            for i, (name, k) in enumerate(zip(NAMES, numbers))
        }

    reg_loads, site_loads = loads(REG_INPUTS, box["reg_in"]), loads(SITE_INPUTS, box["site_in"])
    first = ("nodes", "recv", "spot", "table", "coefs", "disp", "vel", "minv", "send", "fill", "stiff")

    @pl.when(jnp.logical_not(is_site))
    def _():
        for name in first:
            if name in reg_loads:
                reg_loads[name].start()

    @pl.when(is_site)
    def _():
        for name in first:
            site_loads[name].start()

    barrier = pltpu.get_barrier_semaphore()

    def greet(target):
        pl.semaphore_signal(barrier, inc=1, device_id=target, device_id_type=MESH)

    for flag, place in ((has_cross, cross), (has_mate, mate), (has_beyond, beyond)):

        @pl.when(flag)
        def _():
            greet((grp, place))

    @pl.when(is_site)
    def _():
        for m in range(3):
            greet((m * sites + part, sub))

    @pl.when(jnp.logical_and(is_site, has_cross))
    def _():
        for m in range(3):
            greet((m * sites + part, cross))

    for name in ("cross_send", "mate_send", "layer_send"):
        b[name][...] = jnp.zeros_like(b[name])

    for flag, names in ((has_cross, ("cross_recv",)), (has_mate, ("mate_recv",)), (has_beyond, ("far_recv",))):

        @pl.when(jnp.logical_not(flag))
        def _():
            for name in names:
                b[name][...] = jnp.zeros_like(b[name])

    lane = lax.broadcasted_iota(jnp.int32, (1, slots), 1)

    def role(site):
        prefix = "site" if site else "reg"
        d = sd if site else rd
        v, gv = box[prefix + "_in"], box[prefix + "_ghost_in"]
        shared, own, ghost = box[prefix + "_shared"], dict(box[prefix + "_own"]), dict(box[prefix + "_ghost"])
        for s in (own, ghost):
            s.update(shared)
        load = site_loads if site else reg_loads
        names = SITE_SHARED if site else REG_SHARED
        first_fill = 2 if site else 0
        hp = d["hp"]

        def cross_copy(r):
            return remote(b["cross_send"].at[r], b["cross_recv"].at[r], b["cross_ss"].at[r], b["cross_rs"].at[r], (grp, cross))

        def w_copy(r):
            return remote(own["w_send"].at[r], own["w_recv"].at[r], b["w_ss"].at[r], b["w_rs"].at[r], (grp, cross))

        def mate_copy(n):
            return remote(b["mate_send"].at[n], b["mate_recv"].at[n], b["mate_ss"].at[n], b["mate_rs"].at[n], (grp, mate))

        def far_copy(r, target):
            return remote(b["mate_send"].at[2 * r], b["far_recv"].at[r], b["far_ss"].at[r], b["far_rs"].at[r], (grp, target))

        def share_copy(k):
            return remote(v[names[k]], gv[names[k]], b["share_ss"].at[k], b["share_rs"].at[k], (grp, cross))

        def layer_copy(n, m):
            return remote(
                b["layer_send"].at[n], b["layer_recv"].at[n, m], b["layer_ss"].at[n], b["layer_rs"].at[n, m],
                (regs + part, sub),
            )

        def layer_ghost(r, m):
            return remote(
                b["layer_send"].at[2 * r], b["layer_far"].at[r, m], b["layer_gs"].at[r], b["layer_gr"].at[r, m],
                (regs + part, cross),
            )

        def limit(fills, side):
            low, high = (fills[0, :, first_fill + k : first_fill + k + 1] for k in range(2))
            return jnp.where(side == 0, low, high)

        def row(ref, side):
            return ref[pl.ds(side, 1), :]

        def put(ref, n, rows):
            for c in range(3):
                ref[n, c : c + 1, :] = rows[c]

        def slot_terms(s, maps, blocks, hot):
            left = [spread_block(d, block, index) for block, index in zip(blocks, maps)]
            return join(d, dot(jnp.concatenate(left, axis=1), hot))

        def layer_terms(s, w, ref, n):
            maps = [w["spot"][m] for m in range(3)]
            return slot_terms(s, maps, [ref[n, m] * w["stiff"][m] for m in range(3)], s["slot_hot"][2 * slots :, :])

        def send_layer(n, field):
            put(b["layer_send"], n, pick(d, field, v["spot"][0], lane < layer_fill[...]))
            layer_copy(n, source).start()

        early = names[:3] if site else names[:2]
        for name in early:
            load[name].wait()

        def slot_rows(w, near, far):
            return [row(w["recv"], near), row(w["recv"], far)] + ([w["spot"][m] for m in range(3)] if site else [])

        fill_nodes(d, own, v["nodes"], slot_rows(v, cross_side, mate_side))
        for name in first:
            if name in load and name not in early:
                load[name].wait()

        @pl.when(jnp.logical_not(has_cross))
        def _():
            for name in names:
                gv[name][...] = jnp.zeros_like(gv[name])
            own["w_recv"][...] = jnp.zeros_like(own["w_recv"])
            if site:
                b["layer_far"][...] = jnp.zeros_like(b["layer_far"])

        others = 0 if site else 1 + count(has_cross)
        pl.semaphore_wait(barrier, count(has_cross) + count(has_mate) + count(has_behind) + others)

        @pl.when(has_cross)
        def _():
            for k in range(len(names)):
                share_copy(k).start()

        fill_tables(d, own, v["table"], b["square"])
        fill_matrix(d, own, v["coefs"])
        fill_state(
            d,
            [
                (own["u"], lambda c, cut: v["disp"][c, :, cut]),
                (own["prev"], lambda c, cut: v["disp"][c, :, cut] - v["vel"][c, :, cut]),
                (own["minv"], lambda c, cut: v["minv"][0, :, cut]),
            ],
        )
        near_live = lane < limit(v["fill"], cross_side)
        mate_live = lane < limit(v["fill"], mate_side)

        def ghost_setup():
            @pl.when(has_cross)
            def _():
                for k in range(len(names)):
                    share_copy(k).wait_recv()

            fill_nodes(d, ghost, gv["nodes"], slot_rows(gv, mate_side, cross_side))
            fill_matrix(d, ghost, gv["coefs"])
            fill_state(d, [(ghost["minv"], lambda c, cut: gv["minv"][0, :, cut])])

        def body(r, carry):
            n = 2 * r
            force = element_forces(d, own)
            put(b["cross_send"], r, pick(d, force, row(v["send"], cross_side), near_live))

            @pl.when(has_cross)
            def _():
                cross_copy(r).start()

            put(b["mate_send"], n, pick(d, force, row(v["send"], mate_side), mate_live))

            @pl.when(has_mate)
            def _():
                mate_copy(n).start()

            @pl.when(has_behind)
            def _():
                far_copy(r, behind).start()

            now = own["u"][...]
            ahead = 2.0 * now - own["prev"][...] + own["minv"][...] * force
            own["w_send"][r] = ahead

            @pl.when(has_cross)
            def _():
                w_copy(r).start()

            pl.when(r == 0)(ghost_setup)

            extra = jnp.zeros_like(force)
            if site:
                for m in range(3):
                    layer_copy(n, m).wait_recv()
                extra = layer_terms(own, v, b["layer_recv"], n)

            @pl.when(has_mate)
            def _():
                mate_copy(n).wait_recv()

            @pl.when(has_cross)
            def _():
                cross_copy(r).wait_recv()

            maps = [row(v["recv"], cross_side), row(v["recv"], mate_side)]
            hot = own["slot_hot"][0 : 2 * slots, :]
            extra = extra + slot_terms(own, maps, [b["cross_recv"][r], b["mate_recv"][n]], hot)
            middle = ahead + own["minv"][...] * extra
            own["prev"][...] = now
            own["u"][...] = middle
            if not site:
                send_layer(n, middle)

                @pl.when(has_cross)
                def _():
                    layer_ghost(r, source).start()

            force = element_forces(d, own)
            put(b["mate_send"], n + 1, pick(d, force, row(v["send"], mate_side), mate_live))

            @pl.when(has_mate)
            def _():
                mate_copy(n + 1).start()

            extra = jnp.zeros_like(force)
            if site:

                @pl.when(has_cross)
                def _():
                    for m in range(3):
                        layer_ghost(r, m).wait_recv()

                extra = layer_terms(ghost, gv, b["layer_far"], r)

            @pl.when(has_beyond)
            def _():
                far_copy(r, beyond).wait_recv()

            @pl.when(has_cross)
            def _():
                w_copy(r).wait_recv()

            ghost_maps = [row(gv["recv"], mate_side), row(gv["recv"], cross_side)]
            hot = ghost["slot_hot"][0 : 2 * slots, :]
            extra = extra + slot_terms(ghost, ghost_maps, [b["cross_send"][r], b["far_recv"][r]], hot)
            ghost["u"][...] = own["w_recv"][r] + ghost["minv"][...] * extra
            ghost_force = element_forces(d, ghost)
            ghost_live = lane < limit(gv["fill"], mate_side)
            near = jnp.concatenate(pick(d, ghost_force, row(gv["send"], mate_side), ghost_live), axis=0)

            extra = force
            if site:
                for m in range(3):
                    layer_copy(n + 1, m).wait_recv()
                extra = extra + layer_terms(own, v, b["layer_recv"], n + 1)

            @pl.when(has_mate)
            def _():
                mate_copy(n + 1).wait_recv()

            hot = own["slot_hot"][0 : 2 * slots, :]
            extra = extra + slot_terms(own, maps, [near, b["mate_recv"][n + 1]], hot)
            later = 2.0 * middle - now + own["minv"][...] * extra
            own["prev"][...] = middle
            own["u"][...] = later
            if not site:
                send_layer(n + 1, later)
            return carry

        lax.fori_loop(0, ROUNDS, body, 0)
        out = site_out if site else reg_out
        for c in range(3):
            for h in range(d["h"]):
                at, size = c * hp + h, min(d["width"], d["count"] - h * d["width"])
                out[c, :, h * d["width"] : h * d["width"] + size] = own["u"][at : at + 1, 0:size]

        def drain(r, carry):
            @pl.when(has_cross)
            def _():
                cross_copy(r).wait_send()
                w_copy(r).wait_send()

            @pl.when(has_behind)
            def _():
                far_copy(r, behind).wait_send()

            for n in (2 * r, 2 * r + 1):

                @pl.when(has_mate)
                def _():
                    mate_copy(n).wait_send()

                if not site:
                    layer_copy(n, source).wait_send()

            if not site:

                @pl.when(has_cross)
                def _():
                    layer_ghost(r, source).wait_send()

            return carry

        lax.fori_loop(0, ROUNDS, drain, 0)

        @pl.when(has_cross)
        def _():
            for k in range(len(names)):
                share_copy(k).wait_send()

    @pl.when(jnp.logical_not(is_site))
    def _():
        site_out[...] = jnp.zeros_like(site_out)
        role(False)

    @pl.when(is_site)
    def _():
        reg_out[...] = jnp.zeros_like(reg_out)
        role(True)


def solution(mesh):
    n_grp, n_sub = mesh.shape["grp"], mesh.shape["sub"]

    def shards(*args):
        args = list(args)
        for k in (0, 1, 2, 3, 4, 5, 19, 20):
            rows, length = args[k].shape[2:]
            args[k] = jnp.transpose(args[k], (0, 2, 1, 3)).reshape(rows, 1, length)
        for k in (12, 13, 14, 15):
            args[k] = args[k].reshape(args[k].shape[2:])
        args[9] = args[9].T
        for k in (6, 7):
            args[k] = args[k].reshape((9,) + args[k].shape[4:])
        rd = sizes(args[4].shape, args[6].shape, args[0].shape)
        sd = sizes(args[5].shape, args[7].shape, args[2].shape)
        slots = args[12].shape[1]
        vmem = pl.BlockSpec(memory_space=pltpu.VMEM)
        hbm = pl.BlockSpec(memory_space=pltpu.HBM)
        dma = pltpu.SemaphoreType.DMA
        block = (8, slots)
        groups = {
            "common": dict(
                square=pltpu.VMEM((LANES, LANES), F32),
                cross_send=pltpu.VMEM((ROUNDS,) + block, F32),
                cross_recv=pltpu.VMEM((ROUNDS,) + block, F32),
                mate_send=pltpu.VMEM((STEPS,) + block, F32),
                mate_recv=pltpu.VMEM((STEPS,) + block, F32),
                far_recv=pltpu.VMEM((ROUNDS,) + block, F32),
                layer_send=pltpu.VMEM((STEPS,) + block, F32),
                layer_recv=pltpu.VMEM((STEPS, 3) + block, F32),
                layer_far=pltpu.VMEM((ROUNDS, 3) + block, F32),
                load_sem=dma((len(SITE_INPUTS),)),
                cross_ss=dma((ROUNDS,)),
                cross_rs=dma((ROUNDS,)),
                w_ss=dma((ROUNDS,)),
                w_rs=dma((ROUNDS,)),
                mate_ss=dma((STEPS,)),
                mate_rs=dma((STEPS,)),
                far_ss=dma((ROUNDS,)),
                far_rs=dma((ROUNDS,)),
                layer_ss=dma((STEPS,)),
                layer_rs=dma((STEPS, 3)),
                layer_gs=dma((ROUNDS,)),
                layer_gr=dma((ROUNDS, 3)),
                share_ss=dma((len(SITE_SHARED),)),
                share_rs=dma((len(SITE_SHARED),)),
            )
        }
        for prefix, d, numbers, shared, slot_rows in (
            ("reg", rd, REG_INPUTS, REG_SHARED, 2),
            ("site", sd, SITE_INPUTS, SITE_SHARED, 5),
        ):
            places = {name: pltpu.VMEM(args[k].shape, args[k].dtype) for name, k in zip(NAMES, numbers)}
            groups[prefix + "_in"] = places
            groups[prefix + "_ghost_in"] = {name: places[name] for name in shared}
            groups[prefix + "_shared"] = role_scratch(d, slots)
            groups[prefix + "_own"] = part_scratch(d, slot_rows, slots)
            groups[prefix + "_ghost"] = part_scratch(d, slot_rows, slots)
        keys = [(group, list(items)) for group, items in groups.items()]
        reg_out, site_out = pl.pallas_call(
            functools.partial(kernel, n_grp, n_sub, rd, sd, slots, keys),
            out_shape=(
                jax.ShapeDtypeStruct(args[0].shape, F32),
                jax.ShapeDtypeStruct(args[2].shape, F32),
            ),
            in_specs=[vmem if k == SCALAR else hbm for k in range(len(args))],
            out_specs=(vmem, vmem),
            scratch_shapes=[place for items in groups.values() for place in items.values()],
            compiler_params=pltpu.CompilerParams(
                collective_id=0, has_side_effects=True, vmem_limit_bytes=32 * 1024 * 1024
            ),
        )(*[arg if k == SCALAR else pltpu.with_memory_space_constraint(arg, pltpu.HBM) for k, arg in enumerate(args)])
        return tuple(out.reshape(1, 1, out.shape[0], out.shape[2]) for out in (reg_out, site_out))

    cell = ("grp", "sub")
    specs = [P(*cell)] * 21
    specs[8] = specs[9] = P()
    return jax.shard_map(
        shards,
        mesh=mesh,
        in_specs=tuple(specs),
        out_specs=(P(*cell), P(*cell)),
        check_vma=False,
    )
```

```python
import functools

import jax
import jax.numpy as jnp
from jax import lax
from jax.experimental import pallas as pl
from jax.experimental.pallas import tpu as pltpu
from jax.sharding import PartitionSpec as P

STEPS = 8
ROUNDS = STEPS // 2
LANES = 128
MESH = pl.DeviceIdType.MESH
F32 = jnp.float32
BF16 = jnp.bfloat16


def up(size, unit):
    return -(-size // unit) * unit


def lane_gather(block, index):
    numbers = lax.GatherDimensionNumbers(
        offset_dims=(),
        collapsed_slice_dims=(1,),
        start_index_map=(1,),
        operand_batching_dims=(0,),
        start_indices_batching_dims=(0,),
    )
    return lax.gather(
        block,
        index[..., None],
        numbers,
        slice_sizes=(1, 1),
        mode=lax.GatherScatterMode.PROMISE_IN_BOUNDS,
    )


def split(value):
    high = value.astype(BF16)
    low = (value - high.astype(F32)).astype(BF16)
    return high, low


def dot(left, right):
    return jnp.dot(left, right, preferred_element_type=F32)


def sizes(nodes_shape, coefs_shape, disp_shape):
    p, _, e = nodes_shape
    q = coefs_shape[-2]
    count = disp_shape[-1]
    width = LANES
    h = -(-count // width)
    qp = up(q, 8)
    return dict(
        p=p, e=e, q=q, count=count, width=width, shift=width.bit_length() - 1, h=h, hp=up(h, 8), qp=qp,
        p8=up(p, 8), kw=up(9 * qp, LANES),
    )


def part_scratch(d, slot_rows, slots):
    state = (3 * d["hp"], d["width"])
    return dict(
        lane=pltpu.VMEM((d["p8"], d["e"]), jnp.int32),
        block=pltpu.VMEM((d["p8"], d["e"]), jnp.int32),
        hot=pltpu.VMEM((d["p"] * d["e"], d["width"]), BF16),
        slot_hot=pltpu.VMEM((slot_rows * slots, d["width"]), BF16),
        fe=pltpu.VMEM((2, d["p8"], 3 * d["e"]), F32),
        ve=pltpu.VMEM((3, d["p8"], d["e"]), F32),
        matrix=pltpu.VMEM((d["p"] * d["p8"], d["e"]), F32),
        u=pltpu.VMEM(state, F32),
        minv=pltpu.VMEM(state, F32),
    )


def role_scratch(d, slots):
    state = (3 * d["hp"], d["width"])
    return dict(
        wide=pltpu.VMEM((2, d["p8"], d["kw"]), F32),
        weight=pltpu.VMEM((2, up(d["p"] * d["p8"], 16), d["kw"]), BF16),
        cube=pltpu.VMEM((9 * d["qp"], d["e"]), F32),
        turn=pltpu.VMEM((LANES, max(d["e"], slots)), F32),
        prev=pltpu.VMEM(state, F32),
        force=pltpu.VMEM(state, F32),
        w_send=pltpu.VMEM((ROUNDS,) + state, F32),
        w_recv=pltpu.VMEM((ROUNDS,) + state, F32),
    )


def fill_onehot(d, out_ref, rows, turn):
    length = rows[0].shape[1]
    for r, row in enumerate(rows):
        turn[r : r + 1, 0:length] = (row & (d["width"] - 1)).astype(F32)
    columns = turn[:, 0:length].T
    lane = lax.broadcasted_iota(jnp.int32, (length, d["width"]), 1).astype(F32)
    for r in range(len(rows)):
        hot = jnp.where(lane == columns[:, r : r + 1], 1.0, 0.0)
        out_ref[r * length : (r + 1) * length, :] = hot.astype(BF16)


def fill_tables(d, s, table, square):
    p, q, qp, p8 = d["p"], d["q"], d["qp"], d["p8"]
    wide = s["wide"]
    wide[...] = jnp.zeros_like(wide)
    if table.shape[0] != p:
        square[...] = jnp.zeros_like(square)
        square[0 : 3 * q, 0:p] = table[...]
        square[...] = square[...].T
        table = square
    for a in range(3):
        for b in range(3):
            at = (3 * a + b) * qp
            wide[0, 0:p, at : at + q] = table[0:p, a * q : (a + 1) * q]
            wide[1, 0:p, at : at + q] = table[0:p, b * q : (b + 1) * q]
    left = -wide[0]
    for first in range(0, p, 2):
        rows = range(first, min(p, first + 2))
        high, low = split(jnp.concatenate([left * wide[1, n : n + 1, :] for n in rows], axis=0))
        cut = slice(first * p8, (rows[-1] + 1) * p8)
        s["weight"][0, cut, :] = high
        s["weight"][1, cut, :] = low


def fill_nodes(d, s, nodes, slot_rows):
    p = d["p"]
    s["lane"][...] = jnp.zeros_like(s["lane"])
    s["block"][...] = jnp.full_like(s["block"], -1)
    for r in range(p):
        s["lane"][r : r + 1, :] = nodes[r] & (LANES - 1)
        s["block"][r : r + 1, :] = nodes[r] >> 7
    s["turn"][...] = jnp.zeros_like(s["turn"])
    fill_onehot(d, s["hot"], [nodes[r] for r in range(p)], s["turn"])
    fill_onehot(d, s["slot_hot"], slot_rows, s["turn"])


def fill_state(d, pairs):
    hp, width, count = d["hp"], d["width"], d["count"]
    for ref, _ in pairs:
        ref[...] = jnp.zeros_like(ref)
    for c in range(3):
        for h in range(d["h"]):
            size = min(width, count - h * width)
            at, cut = c * hp + h, slice(h * width, h * width + size)
            for ref, value in pairs:
                ref[at : at + 1, 0:size] = value(c, cut)


def fill_matrix(d, s, coefs):
    q, qp, p, p8, e, depth = d["q"], d["qp"], d["p"], d["p8"], d["e"], 9 * d["qp"]
    if qp != q:
        s["cube"][...] = jnp.zeros_like(s["cube"])
    for k in range(9):
        s["cube"][k * qp : k * qp + q, :] = coefs[k]
    high, low = split(s["cube"][...])
    both = jnp.concatenate([high, low], axis=1)
    for first in range(0, p, 2):
        cut = slice(first * p8, min(p, first + 2) * p8)
        wide = dot(s["weight"][0, cut, 0:depth], both)
        s["matrix"][cut, :] = wide[:, 0:e] + wide[:, e:] + dot(s["weight"][1, cut, 0:depth], high)


def spread(d, rows, blocks):
    lanes = rows[0].shape[1]
    mine = lax.broadcasted_iota(jnp.int32, (d["hp"], lanes), 0) == blocks
    return jnp.concatenate([jnp.where(mine, row, 0.0) for row in rows], axis=0).astype(BF16)


def spread_block(d, block, index):
    high = block.astype(BF16).astype(F32)
    low = block - high
    rows = [part[c : c + 1] for part in (high, low) for c in range(3)]
    return spread(d, rows, index >> d["shift"])


def join(d, total):
    half = 3 * d["hp"]
    return total[0:half] + total[half:]


def pick(d, field, index, live):
    hp, slots = d["hp"], index.shape[1]
    lane = jnp.broadcast_to(index & (LANES - 1), (hp, slots))
    blocks = jnp.where(live, index >> d["shift"], -1)
    mine = lax.broadcasted_iota(jnp.int32, (hp, slots), 0) == blocks
    parts = d["width"] // LANES
    which = jnp.broadcast_to((index >> 7) & (parts - 1), (hp, slots))
    out = []
    for c in range(3):
        rows = field[c * hp : (c + 1) * hp]
        got = lane_gather(rows[:, 0:LANES], lane)
        for k in range(1, parts):
            got = jnp.where(which == k, lane_gather(rows[:, k * LANES : (k + 1) * LANES], lane), got)
        out.append(jnp.sum(jnp.where(mine, got, 0.0), axis=0, keepdims=True))
    return out


def element_forces(d, s):
    p, e, p8, hp = d["p"], d["e"], d["p8"], d["hp"]
    parts = d["width"] // LANES
    blocks128 = -(-d["count"] // LANES)
    groups = p8 // 8
    for t in range(e // LANES):
        cut = slice(t * LANES, (t + 1) * LANES)
        for g in range(groups):
            lane = s["lane"][8 * g : 8 * g + 8, cut]
            block = s["block"][8 * g : 8 * g + 8, cut]
            bits = [(block >> k) & 1 == 1 for k in range((blocks128 - 1).bit_length())]
            for c in range(3):
                values = []
                for h in range(blocks128):
                    at, part = h // parts, h % parts
                    row = s["u"][c * hp + at : c * hp + at + 1, part * LANES : (part + 1) * LANES]
                    values.append(lane_gather(jnp.broadcast_to(row, (8, LANES)), lane))
                for bit in bits:
                    values = [
                        jnp.where(bit, values[k + 1], values[k]) if k + 1 < len(values) else values[k]
                        for k in range(0, len(values), 2)
                    ]
                s["ve"][c, 8 * g : 8 * g + 8, cut] = values[0]
        total = [[None] * groups for _ in range(3)]
        for n in range(p):
            rows = [s["ve"][c, n : n + 1, cut] for c in range(3)]
            for g in range(groups):
                weight = s["matrix"][n * p8 + 8 * g : n * p8 + 8 * g + 8, cut]
                for c in range(3):
                    term = weight * rows[c]
                    total[c][g] = term if n == 0 else total[c][g] + term
        for g in range(groups):
            for c in range(3):
                high = total[c][g].astype(BF16).astype(F32)
                at = slice(c * e + t * LANES, c * e + (t + 1) * LANES)
                s["fe"][0, 8 * g : 8 * g + 8, at] = high
                s["fe"][1, 8 * g : 8 * g + 8, at] = total[c][g] - high
    up_shift = parts.bit_length() - 1
    step = max(1, 2 * LANES // e)
    total = None
    for first in range(0, p, step):
        chunk = range(first, min(p, first + step))
        left = []
        for n in chunk:
            rows = [s["fe"][k, n : n + 1, c * e : (c + 1) * e] for k in range(2) for c in range(3)]
            left.append(spread(d, rows, s["block"][n : n + 1, :] >> up_shift))
        piece = dot(jnp.concatenate(left, axis=1), s["hot"][first * e : (chunk[-1] + 1) * e, :])
        total = piece if total is None else total + piece
    return join(d, total)


SCALAR = 18
REG_INPUTS = (0, 1, 4, 6, 8, 10, 12, 13, 16, 17)
SITE_INPUTS = (2, 3, 5, 7, 9, 11, 14, 15, 16, 19, 20)
NAMES = ("disp", "vel", "nodes", "coefs", "table", "minv", "send", "recv", "fill", "spot", "stiff")
REG_SHARED = ("nodes", "recv", "send", "fill", "minv", "coefs")
SITE_SHARED = ("nodes", "recv", "spot", "send", "fill", "minv", "stiff", "coefs")


def kernel(n_grp, n_sub, rd, sd, slots, keys, *refs):
    inputs, (reg_out, site_out), refs = refs[:21], refs[21:23], refs[23:]
    layer_fill = inputs[SCALAR]
    box = {}
    for group, names in keys:
        box[group], refs = dict(zip(names, refs)), refs[len(names) :]
    b = box["common"]
    sites = n_grp // 4
    regs = 3 * sites
    grp, sub = lax.axis_index("grp"), lax.axis_index("sub")
    is_site = grp >= regs
    source, part = grp // sites, grp % sites
    odd = lax.rem(sub, 2)
    cross_side, mate_side = odd, 1 - odd
    way = 2 * odd - 1
    cross, mate, beyond, behind = sub + way, sub - way, sub + 2 * way, sub - 2 * way

    def exists(place):
        return jnp.logical_and(place >= 0, place < n_sub)

    has_cross, has_mate, has_beyond, has_behind = (exists(place) for place in (cross, mate, beyond, behind))

    def count(flag):
        return jnp.where(flag, 1, 0)

    def remote(src, dst, send_sem, recv_sem, target):
        return pltpu.make_async_remote_copy(
            src_ref=src, dst_ref=dst, send_sem=send_sem, recv_sem=recv_sem, device_id=target, device_id_type=MESH
        )

    def loads(numbers, places):
        return {
            name: pltpu.make_async_copy(inputs[k], places[name], b["load_sem"].at[i])
            for i, (name, k) in enumerate(zip(NAMES, numbers))
        }

    reg_loads, site_loads = loads(REG_INPUTS, box["reg_in"]), loads(SITE_INPUTS, box["site_in"])
    first = ("nodes", "recv", "spot", "table", "coefs", "disp", "vel", "minv", "send", "fill", "stiff")

    @pl.when(jnp.logical_not(is_site))
    def _():
        for name in first:
            if name in reg_loads:
                reg_loads[name].start()

    @pl.when(is_site)
    def _():
        for name in first:
            site_loads[name].start()

    barrier = pltpu.get_barrier_semaphore()

    def greet(target):
        pl.semaphore_signal(barrier, inc=1, device_id=target, device_id_type=MESH)

    for flag, place in ((has_cross, cross), (has_mate, mate), (has_beyond, beyond)):

        @pl.when(flag)
        def _():
            greet((grp, place))

    @pl.when(is_site)
    def _():
        for m in range(3):
            greet((m * sites + part, sub))

    @pl.when(jnp.logical_and(is_site, has_cross))
    def _():
        for m in range(3):
            greet((m * sites + part, cross))

    for name in ("cross_send", "mate_send", "layer_send"):
        b[name][...] = jnp.zeros_like(b[name])

    for flag, names in ((has_cross, ("cross_recv",)), (has_mate, ("mate_recv",)), (has_beyond, ("far_recv",))):

        @pl.when(jnp.logical_not(flag))
        def _():
            for name in names:
                b[name][...] = jnp.zeros_like(b[name])

    lane = lax.broadcasted_iota(jnp.int32, (1, slots), 1)

    def role(site):
        prefix = "site" if site else "reg"
        d = sd if site else rd
        v, gv = box[prefix + "_in"], box[prefix + "_ghost_in"]
        shared, own, ghost = box[prefix + "_shared"], dict(box[prefix + "_own"]), dict(box[prefix + "_ghost"])
        for s in (own, ghost):
            s.update(shared)
        load = site_loads if site else reg_loads
        names = SITE_SHARED if site else REG_SHARED
        first_fill = 2 if site else 0
        hp = d["hp"]

        def cross_copy(r):
            return remote(b["cross_send"].at[r], b["cross_recv"].at[r], b["cross_ss"].at[r], b["cross_rs"].at[r], (grp, cross))

        def w_copy(r):
            return remote(own["w_send"].at[r], own["w_recv"].at[r], b["w_ss"].at[r], b["w_rs"].at[r], (grp, cross))

        def mate_copy(n):
            return remote(b["mate_send"].at[n], b["mate_recv"].at[n], b["mate_ss"].at[n], b["mate_rs"].at[n], (grp, mate))

        def far_copy(r, target):
            return remote(b["mate_send"].at[2 * r], b["far_recv"].at[r], b["far_ss"].at[r], b["far_rs"].at[r], (grp, target))

        def share_copy(k):
            return remote(v[names[k]], gv[names[k]], b["share_ss"].at[k], b["share_rs"].at[k], (grp, cross))

        def layer_copy(n, m):
            return remote(
                b["layer_send"].at[n], b["layer_recv"].at[n, m], b["layer_ss"].at[n], b["layer_rs"].at[n, m],
                (regs + part, sub),
            )

        def layer_ghost(r, m):
            return remote(
                b["layer_send"].at[2 * r], b["layer_far"].at[r, m], b["layer_gs"].at[r], b["layer_gr"].at[r, m],
                (regs + part, cross),
            )

        def limit(fills, side):
            low, high = (fills[0, :, first_fill + k : first_fill + k + 1] for k in range(2))
            return jnp.where(side == 0, low, high)

        def row(ref, side):
            return ref[pl.ds(side, 1), :]

        def put(ref, n, rows):
            for c in range(3):
                ref[n, c : c + 1, :] = rows[c]

        def slot_terms(s, maps, blocks, hot):
            left = [spread_block(d, block, index) for block, index in zip(blocks, maps)]
            return join(d, dot(jnp.concatenate(left, axis=1), hot))

        def layer_terms(s, w, ref, n):
            maps = [w["spot"][m] for m in range(3)]
            return slot_terms(s, maps, [ref[n, m] * w["stiff"][m] for m in range(3)], s["slot_hot"][2 * slots :, :])

        def send_layer(n, field):
            put(b["layer_send"], n, pick(d, field, v["spot"][0], lane < layer_fill[...]))
            layer_copy(n, source).start()

        early = names[:3] if site else names[:2]
        for name in early:
            load[name].wait()

        def slot_rows(w, near, far):
            return [row(w["recv"], near), row(w["recv"], far)] + ([w["spot"][m] for m in range(3)] if site else [])

        fill_nodes(d, own, v["nodes"], slot_rows(v, cross_side, mate_side))
        for name in first:
            if name in load and name not in early:
                load[name].wait()

        @pl.when(jnp.logical_not(has_cross))
        def _():
            for name in names:
                gv[name][...] = jnp.zeros_like(gv[name])
            own["w_recv"][...] = jnp.zeros_like(own["w_recv"])
            if site:
                b["layer_far"][...] = jnp.zeros_like(b["layer_far"])

        def meet_and_share():
            others = 0 if site else 1 + count(has_cross)
            pl.semaphore_wait(barrier, count(has_cross) + count(has_mate) + count(has_behind) + others)

            @pl.when(has_cross)
            def _():
                for k in range(len(names)):
                    share_copy(k).start()

        if site:
            meet_and_share()
        fill_tables(d, own, v["table"], b["square"])
        fill_matrix(d, own, v["coefs"])
        fill_state(
            d,
            [
                (own["u"], lambda c, cut: v["disp"][c, :, cut]),
                (own["prev"], lambda c, cut: v["disp"][c, :, cut] - v["vel"][c, :, cut]),
                (own["minv"], lambda c, cut: v["minv"][0, :, cut]),
            ],
        )
        near_live = lane < limit(v["fill"], cross_side)
        mate_live = lane < limit(v["fill"], mate_side)

        def ghost_setup():
            @pl.when(has_cross)
            def _():
                for k in range(len(names)):
                    share_copy(k).wait_recv()

            fill_nodes(d, ghost, gv["nodes"], slot_rows(gv, mate_side, cross_side))
            fill_matrix(d, ghost, gv["coefs"])
            fill_state(d, [(ghost["minv"], lambda c, cut: gv["minv"][0, :, cut])])

        def body(r, carry):
            n = 2 * r
            force = own["force"][...]
            put(b["cross_send"], r, pick(d, force, row(v["send"], cross_side), near_live))

            @pl.when(has_cross)
            def _():
                cross_copy(r).start()

            put(b["mate_send"], n, pick(d, force, row(v["send"], mate_side), mate_live))

            @pl.when(has_mate)
            def _():
                mate_copy(n).start()

            @pl.when(has_behind)
            def _():
                far_copy(r, behind).start()

            now = own["u"][...]
            ahead = 2.0 * now - own["prev"][...] + own["minv"][...] * force
            own["w_send"][r] = ahead

            @pl.when(has_cross)
            def _():
                w_copy(r).start()

            pl.when(r == 0)(ghost_setup)

            extra = ghost_extra = jnp.zeros_like(force)
            if site:
                for m in range(3):
                    layer_copy(n, m).wait_recv()

                @pl.when(has_cross)
                def _():
                    for m in range(3):
                        layer_ghost(r, m).wait_recv()

                extra = layer_terms(own, v, b["layer_recv"], n)
                ghost_extra = layer_terms(ghost, gv, b["layer_far"], r)

            @pl.when(has_mate)
            def _():
                mate_copy(n).wait_recv()

            @pl.when(has_cross)
            def _():
                cross_copy(r).wait_recv()

            maps = [row(v["recv"], cross_side), row(v["recv"], mate_side)]
            hot = own["slot_hot"][0 : 2 * slots, :]
            extra = extra + slot_terms(own, maps, [b["cross_recv"][r], b["mate_recv"][n]], hot)
            middle = ahead + own["minv"][...] * extra
            own["prev"][...] = now
            own["u"][...] = middle
            if not site:
                send_layer(n, middle)

                @pl.when(has_cross)
                def _():
                    layer_ghost(r, source).start()

            force = element_forces(d, own)
            put(b["mate_send"], n + 1, pick(d, force, row(v["send"], mate_side), mate_live))

            @pl.when(has_mate)
            def _():
                mate_copy(n + 1).start()

            extra = ghost_extra

            @pl.when(has_beyond)
            def _():
                far_copy(r, beyond).wait_recv()

            @pl.when(has_cross)
            def _():
                w_copy(r).wait_recv()

            ghost_maps = [row(gv["recv"], mate_side), row(gv["recv"], cross_side)]
            hot = ghost["slot_hot"][0 : 2 * slots, :]
            extra = extra + slot_terms(ghost, ghost_maps, [b["cross_send"][r], b["far_recv"][r]], hot)
            ghost["u"][...] = own["w_recv"][r] + ghost["minv"][...] * extra
            ghost_force = element_forces(d, ghost)
            ghost_live = lane < limit(gv["fill"], mate_side)
            near = jnp.concatenate(pick(d, ghost_force, row(gv["send"], mate_side), ghost_live), axis=0)

            extra = force
            if site:
                for m in range(3):
                    layer_copy(n + 1, m).wait_recv()
                extra = extra + layer_terms(own, v, b["layer_recv"], n + 1)

            @pl.when(has_mate)
            def _():
                mate_copy(n + 1).wait_recv()

            hot = own["slot_hot"][0 : 2 * slots, :]
            extra = extra + slot_terms(own, maps, [near, b["mate_recv"][n + 1]], hot)
            later = 2.0 * middle - now + own["minv"][...] * extra
            own["prev"][...] = middle
            own["u"][...] = later
            if not site:
                send_layer(n + 1, later)

            @pl.when(r < ROUNDS - 1)
            def _():
                own["force"][...] = element_forces(d, own)

            return carry

        own["force"][...] = element_forces(d, own)
        if not site:
            meet_and_share()
        lax.fori_loop(0, ROUNDS, body, 0)
        out = site_out if site else reg_out
        for c in range(3):
            for h in range(d["h"]):
                at, size = c * hp + h, min(d["width"], d["count"] - h * d["width"])
                out[c, :, h * d["width"] : h * d["width"] + size] = own["u"][at : at + 1, 0:size]

        def drain(r, carry):
            @pl.when(has_cross)
            def _():
                cross_copy(r).wait_send()
                w_copy(r).wait_send()

            @pl.when(has_behind)
            def _():
                far_copy(r, behind).wait_send()

            for n in (2 * r, 2 * r + 1):

                @pl.when(has_mate)
                def _():
                    mate_copy(n).wait_send()

                if not site:
                    layer_copy(n, source).wait_send()

            if not site:

                @pl.when(has_cross)
                def _():
                    layer_ghost(r, source).wait_send()

            return carry

        lax.fori_loop(0, ROUNDS, drain, 0)

        @pl.when(has_cross)
        def _():
            for k in range(len(names)):
                share_copy(k).wait_send()

    @pl.when(jnp.logical_not(is_site))
    def _():
        site_out[...] = jnp.zeros_like(site_out)
        role(False)

    @pl.when(is_site)
    def _():
        reg_out[...] = jnp.zeros_like(reg_out)
        role(True)


def write_out(reg_in, site_in, reg_out, site_out, sem):
    copies = [
        pltpu.make_async_copy(src, dst, sem.at[k]) for k, (src, dst) in enumerate(((site_in, site_out), (reg_in, reg_out)))
    ]
    for copy in copies:
        copy.start()
    for copy in copies:
        copy.wait()


def solution(mesh):
    n_grp, n_sub = mesh.shape["grp"], mesh.shape["sub"]

    def shards(*args):
        args = list(args)
        for k in (0, 1, 2, 3, 4, 5, 19, 20):
            rows, length = args[k].shape[2:]
            args[k] = jnp.transpose(args[k], (0, 2, 1, 3)).reshape(rows, 1, length)
        for k in (12, 13, 14, 15):
            args[k] = args[k].reshape(args[k].shape[2:])
        args[9] = args[9].T
        for k in (6, 7):
            args[k] = args[k].reshape((9,) + args[k].shape[4:])
        rd = sizes(args[4].shape, args[6].shape, args[0].shape)
        sd = sizes(args[5].shape, args[7].shape, args[2].shape)
        slots = args[12].shape[1]
        vmem = pl.BlockSpec(memory_space=pltpu.VMEM)
        hbm = pl.BlockSpec(memory_space=pltpu.HBM)
        dma = pltpu.SemaphoreType.DMA
        block = (8, slots)
        groups = {
            "common": dict(
                square=pltpu.VMEM((LANES, LANES), F32),
                cross_send=pltpu.VMEM((ROUNDS,) + block, F32),
                cross_recv=pltpu.VMEM((ROUNDS,) + block, F32),
                mate_send=pltpu.VMEM((STEPS,) + block, F32),
                mate_recv=pltpu.VMEM((STEPS,) + block, F32),
                far_recv=pltpu.VMEM((ROUNDS,) + block, F32),
                layer_send=pltpu.VMEM((STEPS,) + block, F32),
                layer_recv=pltpu.VMEM((STEPS, 3) + block, F32),
                layer_far=pltpu.VMEM((ROUNDS, 3) + block, F32),
                load_sem=dma((len(SITE_INPUTS),)),
                cross_ss=dma((ROUNDS,)),
                cross_rs=dma((ROUNDS,)),
                w_ss=dma((ROUNDS,)),
                w_rs=dma((ROUNDS,)),
                mate_ss=dma((STEPS,)),
                mate_rs=dma((STEPS,)),
                far_ss=dma((ROUNDS,)),
                far_rs=dma((ROUNDS,)),
                layer_ss=dma((STEPS,)),
                layer_rs=dma((STEPS, 3)),
                layer_gs=dma((ROUNDS,)),
                layer_gr=dma((ROUNDS, 3)),
                share_ss=dma((len(SITE_SHARED),)),
                share_rs=dma((len(SITE_SHARED),)),
            )
        }
        for prefix, d, numbers, shared, slot_rows in (
            ("reg", rd, REG_INPUTS, REG_SHARED, 2),
            ("site", sd, SITE_INPUTS, SITE_SHARED, 5),
        ):
            places = {name: pltpu.VMEM(args[k].shape, args[k].dtype) for name, k in zip(NAMES, numbers)}
            groups[prefix + "_in"] = places
            groups[prefix + "_ghost_in"] = {name: places[name] for name in shared}
            groups[prefix + "_shared"] = role_scratch(d, slots)
            groups[prefix + "_own"] = part_scratch(d, slot_rows, slots)
            groups[prefix + "_ghost"] = part_scratch(d, slot_rows, slots)
        keys = [(group, list(items)) for group, items in groups.items()]
        reg_out, site_out = pl.pallas_call(
            functools.partial(kernel, n_grp, n_sub, rd, sd, slots, keys),
            out_shape=(
                jax.ShapeDtypeStruct(args[0].shape, F32),
                jax.ShapeDtypeStruct(args[2].shape, F32),
            ),
            in_specs=[vmem if k == SCALAR else hbm for k in range(len(args))],
            out_specs=(vmem, vmem),
            scratch_shapes=[place for items in groups.values() for place in items.values()],
            compiler_params=pltpu.CompilerParams(
                collective_id=0, has_side_effects=True, vmem_limit_bytes=32 * 1024 * 1024
            ),
        )(*[arg if k == SCALAR else pltpu.with_memory_space_constraint(arg, pltpu.HBM) for k, arg in enumerate(args)])
        outs = (reg_out, site_out)
        outs = pl.pallas_call(
            write_out,
            out_shape=tuple(jax.ShapeDtypeStruct(out.shape, F32) for out in outs),
            in_specs=[vmem] * 2,
            out_specs=(hbm, hbm),
            scratch_shapes=[dma((2,))],
            compiler_params=pltpu.CompilerParams(vmem_limit_bytes=1024 * 1024),
        )(*outs)
        return tuple(out.reshape(1, 1, out.shape[0], out.shape[2]) for out in outs)

    cell = ("grp", "sub")
    specs = [P(*cell)] * 21
    specs[8] = specs[9] = P()
    return jax.shard_map(
        shards,
        mesh=mesh,
        in_specs=tuple(specs),
        out_specs=(P(*cell), P(*cell)),
        check_vma=False,
    )
```

```python
import functools

import jax
import jax.numpy as jnp
from jax import lax
from jax.experimental import pallas as pl
from jax.experimental.pallas import tpu as pltpu
from jax.sharding import PartitionSpec as P

STEPS = 8
ROUNDS = STEPS // 2
LANES = 128
MESH = pl.DeviceIdType.MESH
F32 = jnp.float32
BF16 = jnp.bfloat16


def up(size, unit):
    return -(-size // unit) * unit


def lane_gather(block, index):
    numbers = lax.GatherDimensionNumbers(
        offset_dims=(),
        collapsed_slice_dims=(1,),
        start_index_map=(1,),
        operand_batching_dims=(0,),
        start_indices_batching_dims=(0,),
    )
    return lax.gather(
        block,
        index[..., None],
        numbers,
        slice_sizes=(1, 1),
        mode=lax.GatherScatterMode.PROMISE_IN_BOUNDS,
    )


def split(value):
    high = value.astype(BF16)
    low = (value - high.astype(F32)).astype(BF16)
    return high, low


def dot(left, right):
    return jnp.dot(left, right, preferred_element_type=F32)


def sizes(nodes_shape, coefs_shape, disp_shape):
    p, _, e = nodes_shape
    q = coefs_shape[-2]
    count = disp_shape[-1]
    width = LANES
    h = -(-count // width)
    qp = up(q, 8)
    return dict(
        p=p, e=e, q=q, count=count, width=width, shift=width.bit_length() - 1, h=h, hp=h, rows=up(3 * h, 8), qp=qp,
        p8=up(p, 8), kw=up(9 * qp, LANES),
    )


def part_scratch(d, slot_rows, slots):
    state = (d["rows"], d["width"])
    return dict(
        lane=pltpu.VMEM((d["p8"], d["e"]), jnp.int32),
        block=pltpu.VMEM((d["p8"], d["e"]), jnp.int32),
        hot=pltpu.VMEM((d["p"] * d["e"], d["width"]), BF16),
        slot_hot=pltpu.VMEM((slot_rows * slots, d["width"]), BF16),
        fe=pltpu.VMEM((2, d["p8"], 3 * d["e"]), F32),
        ve=pltpu.VMEM((3, d["p8"], d["e"]), F32),
        matrix=pltpu.VMEM((d["p"] * d["p8"], d["e"]), F32),
        u=pltpu.VMEM(state, F32),
        minv=pltpu.VMEM(state, F32),
    )


def role_scratch(d, slots):
    state = (d["rows"], d["width"])
    return dict(
        wide=pltpu.VMEM((2, d["p8"], d["kw"]), F32),
        weight=pltpu.VMEM((2, up(d["p"] * d["p8"], 16), d["kw"]), BF16),
        cube=pltpu.VMEM((9 * d["qp"], d["e"]), F32),
        turn=pltpu.VMEM((LANES, max(d["e"], slots)), F32),
        prev=pltpu.VMEM(state, F32),
        force=pltpu.VMEM(state, F32),
        w_send=pltpu.VMEM((ROUNDS,) + state, F32),
        w_recv=pltpu.VMEM((ROUNDS,) + state, F32),
    )


def fill_onehot(d, out_ref, rows, turn):
    length = rows[0].shape[1]
    for r, row in enumerate(rows):
        turn[r : r + 1, 0:length] = (row & (d["width"] - 1)).astype(F32)
    columns = turn[:, 0:length].T
    lane = lax.broadcasted_iota(jnp.int32, (length, d["width"]), 1).astype(F32)
    for r in range(len(rows)):
        hot = jnp.where(lane == columns[:, r : r + 1], 1.0, 0.0)
        out_ref[r * length : (r + 1) * length, :] = hot.astype(BF16)


def fill_tables(d, s, table, square):
    p, q, qp, p8 = d["p"], d["q"], d["qp"], d["p8"]
    wide = s["wide"]
    wide[...] = jnp.zeros_like(wide)
    if table.shape[0] != p:
        square[...] = jnp.zeros_like(square)
        square[0 : 3 * q, 0:p] = table[...]
        square[...] = square[...].T
        table = square
    for a in range(3):
        for b in range(3):
            at = (3 * a + b) * qp
            wide[0, 0:p, at : at + q] = table[0:p, a * q : (a + 1) * q]
            wide[1, 0:p, at : at + q] = table[0:p, b * q : (b + 1) * q]
    left = -wide[0]
    for first in range(0, p, 2):
        rows = range(first, min(p, first + 2))
        high, low = split(jnp.concatenate([left * wide[1, n : n + 1, :] for n in rows], axis=0))
        cut = slice(first * p8, (rows[-1] + 1) * p8)
        s["weight"][0, cut, :] = high
        s["weight"][1, cut, :] = low


def fill_nodes(d, s, nodes, slot_rows):
    p = d["p"]
    s["lane"][...] = jnp.zeros_like(s["lane"])
    s["block"][...] = jnp.full_like(s["block"], -1)
    for r in range(p):
        s["lane"][r : r + 1, :] = nodes[r] & (LANES - 1)
        s["block"][r : r + 1, :] = nodes[r] >> 7
    s["turn"][...] = jnp.zeros_like(s["turn"])
    fill_onehot(d, s["hot"], [nodes[r] for r in range(p)], s["turn"])
    fill_onehot(d, s["slot_hot"], slot_rows, s["turn"])


def fill_state(d, pairs):
    hp, width, count = d["hp"], d["width"], d["count"]
    for ref, _ in pairs:
        ref[...] = jnp.zeros_like(ref)
    for c in range(3):
        for h in range(d["h"]):
            size = min(width, count - h * width)
            at, cut = c * hp + h, slice(h * width, h * width + size)
            for ref, value in pairs:
                ref[at : at + 1, 0:size] = value(c, cut)


def fill_matrix(d, s, coefs):
    q, qp, p, p8, e, depth = d["q"], d["qp"], d["p"], d["p8"], d["e"], 9 * d["qp"]
    if qp != q:
        s["cube"][...] = jnp.zeros_like(s["cube"])
    for k in range(9):
        s["cube"][k * qp : k * qp + q, :] = coefs[k]
    high, low = split(s["cube"][...])
    both = jnp.concatenate([high, low], axis=1)
    for first in range(0, p, 2):
        cut = slice(first * p8, min(p, first + 2) * p8)
        wide = dot(s["weight"][0, cut, 0:depth], both)
        s["matrix"][cut, :] = wide[:, 0:e] + wide[:, e:] + dot(s["weight"][1, cut, 0:depth], high)


def spread(d, rows, blocks):
    lanes, hp = rows[0].shape[1], d["hp"]
    place = lax.broadcasted_iota(jnp.int32, (8, lanes), 0)
    out = []
    for k in range(len(rows) // 3):
        for first in range(0, d["rows"], 8):
            value, wanted = None, None
            for c in range(3):
                low, high = c * hp - first, (c + 1) * hp - first
                if high <= 0 or low >= 8:
                    continue
                row, block = jnp.broadcast_to(rows[3 * k + c], (8, lanes)), place - low
                value = row if value is None else jnp.where(place < low, value, row)
                wanted = block if wanted is None else jnp.where(place < low, wanted, block)
            if first + 8 > 3 * hp:
                wanted = jnp.where(place < 3 * hp - first, wanted, -2)
            out.append(jnp.where(wanted == blocks, value, 0.0))
    return jnp.concatenate(out, axis=0).astype(BF16)


def spread_block(d, block, index):
    high = block.astype(BF16).astype(F32)
    low = block - high
    rows = [part[c : c + 1] for part in (high, low) for c in range(3)]
    return spread(d, rows, index >> d["shift"])


def join(d, total):
    half = d["rows"]
    return total[0:half] + total[half:]


def pick(d, field, index, live):
    count, slots = d["rows"], index.shape[1]
    got = lane_gather(field, jnp.broadcast_to(index & (LANES - 1), (count, slots)))
    blocks = jnp.where(live, index >> d["shift"], -4 * count)
    place = lax.broadcasted_iota(jnp.int32, (count, slots), 0)
    return [
        jnp.sum(jnp.where(place == blocks + c * d["hp"], got, 0.0), axis=0, keepdims=True) for c in range(3)
    ]


def element_forces(d, s):
    p, e, p8, hp = d["p"], d["e"], d["p8"], d["hp"]
    parts = d["width"] // LANES
    blocks128 = -(-d["count"] // LANES)
    groups = p8 // 8
    for t in range(e // LANES):
        cut = slice(t * LANES, (t + 1) * LANES)
        for g in range(groups):
            lane = s["lane"][8 * g : 8 * g + 8, cut]
            block = s["block"][8 * g : 8 * g + 8, cut]
            bits = [(block >> k) & 1 == 1 for k in range((blocks128 - 1).bit_length())]
            for c in range(3):
                values = []
                for h in range(blocks128):
                    at, part = h // parts, h % parts
                    row = s["u"][c * hp + at : c * hp + at + 1, part * LANES : (part + 1) * LANES]
                    values.append(lane_gather(jnp.broadcast_to(row, (8, LANES)), lane))
                for bit in bits:
                    values = [
                        jnp.where(bit, values[k + 1], values[k]) if k + 1 < len(values) else values[k]
                        for k in range(0, len(values), 2)
                    ]
                s["ve"][c, 8 * g : 8 * g + 8, cut] = values[0]
        total = [[None] * groups for _ in range(3)]
        for n in range(p):
            rows = [s["ve"][c, n : n + 1, cut] for c in range(3)]
            for g in range(groups):
                weight = s["matrix"][n * p8 + 8 * g : n * p8 + 8 * g + 8, cut]
                for c in range(3):
                    term = weight * rows[c]
                    total[c][g] = term if n == 0 else total[c][g] + term
        for g in range(groups):
            for c in range(3):
                high = total[c][g].astype(BF16).astype(F32)
                at = slice(c * e + t * LANES, c * e + (t + 1) * LANES)
                s["fe"][0, 8 * g : 8 * g + 8, at] = high
                s["fe"][1, 8 * g : 8 * g + 8, at] = total[c][g] - high
    up_shift = parts.bit_length() - 1
    step = max(1, 2 * LANES // e)
    total = None
    for first in range(0, p, step):
        chunk = range(first, min(p, first + step))
        left = []
        for n in chunk:
            rows = [s["fe"][k, n : n + 1, c * e : (c + 1) * e] for k in range(2) for c in range(3)]
            left.append(spread(d, rows, s["block"][n : n + 1, :] >> up_shift))
        piece = dot(jnp.concatenate(left, axis=1), s["hot"][first * e : (chunk[-1] + 1) * e, :])
        total = piece if total is None else total + piece
    return join(d, total)


SCALAR = 18
REG_INPUTS = (0, 1, 4, 6, 8, 10, 12, 13, 16, 17)
SITE_INPUTS = (2, 3, 5, 7, 9, 11, 14, 15, 16, 19, 20)
NAMES = ("disp", "vel", "nodes", "coefs", "table", "minv", "send", "recv", "fill", "spot", "stiff")
REG_SHARED = ("nodes", "recv", "send", "fill", "minv", "coefs")
SITE_SHARED = ("nodes", "recv", "spot", "send", "fill", "minv", "stiff", "coefs")


def kernel(n_grp, n_sub, rd, sd, slots, keys, *refs):
    inputs, (reg_out, site_out), refs = refs[:21], refs[21:23], refs[23:]
    layer_fill = inputs[SCALAR]
    box = {}
    for group, names in keys:
        box[group], refs = dict(zip(names, refs)), refs[len(names) :]
    b = box["common"]
    sites = n_grp // 4
    regs = 3 * sites
    grp, sub = lax.axis_index("grp"), lax.axis_index("sub")
    is_site = grp >= regs
    source, part = grp // sites, grp % sites
    odd = lax.rem(sub, 2)
    cross_side, mate_side = odd, 1 - odd
    way = 2 * odd - 1
    cross, mate, beyond, behind = sub + way, sub - way, sub + 2 * way, sub - 2 * way

    def exists(place):
        return jnp.logical_and(place >= 0, place < n_sub)

    has_cross, has_mate, has_beyond, has_behind = (exists(place) for place in (cross, mate, beyond, behind))

    def count(flag):
        return jnp.where(flag, 1, 0)

    def remote(src, dst, send_sem, recv_sem, target):
        return pltpu.make_async_remote_copy(
            src_ref=src, dst_ref=dst, send_sem=send_sem, recv_sem=recv_sem, device_id=target, device_id_type=MESH
        )

    def loads(numbers, places):
        return {
            name: pltpu.make_async_copy(inputs[k], places[name], b["load_sem"].at[i])
            for i, (name, k) in enumerate(zip(NAMES, numbers))
        }

    reg_loads, site_loads = loads(REG_INPUTS, box["reg_in"]), loads(SITE_INPUTS, box["site_in"])
    first = ("nodes", "recv", "spot", "table", "coefs", "disp", "vel", "minv", "send", "fill", "stiff")

    @pl.when(jnp.logical_not(is_site))
    def _():
        for name in first:
            if name in reg_loads:
                reg_loads[name].start()

    @pl.when(is_site)
    def _():
        for name in first:
            site_loads[name].start()

    barrier = pltpu.get_barrier_semaphore()

    def greet(target):
        pl.semaphore_signal(barrier, inc=1, device_id=target, device_id_type=MESH)

    for flag, place in ((has_cross, cross), (has_mate, mate), (has_beyond, beyond)):

        @pl.when(flag)
        def _():
            greet((grp, place))

    @pl.when(is_site)
    def _():
        for m in range(3):
            greet((m * sites + part, sub))

    @pl.when(jnp.logical_and(is_site, has_cross))
    def _():
        for m in range(3):
            greet((m * sites + part, cross))

    for name in ("cross_send", "mate_send", "layer_send"):
        b[name][...] = jnp.zeros_like(b[name])

    for flag, names in ((has_cross, ("cross_recv",)), (has_mate, ("mate_recv",)), (has_beyond, ("far_recv",))):

        @pl.when(jnp.logical_not(flag))
        def _():
            for name in names:
                b[name][...] = jnp.zeros_like(b[name])

    lane = lax.broadcasted_iota(jnp.int32, (1, slots), 1)

    def role(site):
        prefix = "site" if site else "reg"
        d = sd if site else rd
        v, gv = box[prefix + "_in"], box[prefix + "_ghost_in"]
        shared, own, ghost = box[prefix + "_shared"], dict(box[prefix + "_own"]), dict(box[prefix + "_ghost"])
        for s in (own, ghost):
            s.update(shared)
        load = site_loads if site else reg_loads
        names = SITE_SHARED if site else REG_SHARED
        first_fill = 2 if site else 0
        hp = d["hp"]

        def cross_copy(r):
            return remote(b["cross_send"].at[r], b["cross_recv"].at[r], b["cross_ss"].at[r], b["cross_rs"].at[r], (grp, cross))

        def w_copy(r):
            return remote(own["w_send"].at[r], own["w_recv"].at[r], b["w_ss"].at[r], b["w_rs"].at[r], (grp, cross))

        def mate_copy(n):
            return remote(b["mate_send"].at[n], b["mate_recv"].at[n], b["mate_ss"].at[n], b["mate_rs"].at[n], (grp, mate))

        def far_copy(r, target):
            return remote(b["mate_send"].at[2 * r], b["far_recv"].at[r], b["far_ss"].at[r], b["far_rs"].at[r], (grp, target))

        def share_copy(k):
            return remote(v[names[k]], gv[names[k]], b["share_ss"].at[k], b["share_rs"].at[k], (grp, cross))

        def layer_copy(n, m):
            return remote(
                b["layer_send"].at[n], b["layer_recv"].at[n, m], b["layer_ss"].at[n], b["layer_rs"].at[n, m],
                (regs + part, sub),
            )

        def layer_ghost(r, m):
            return remote(
                b["layer_send"].at[2 * r], b["layer_far"].at[r, m], b["layer_gs"].at[r], b["layer_gr"].at[r, m],
                (regs + part, cross),
            )

        def limit(fills, side):
            low, high = (fills[0, :, first_fill + k : first_fill + k + 1] for k in range(2))
            return jnp.where(side == 0, low, high)

        def row(ref, side):
            return ref[pl.ds(side, 1), :]

        def put(ref, n, rows):
            for c in range(3):
                ref[n, c : c + 1, :] = rows[c]

        def slot_terms(s, maps, blocks, hot):
            left = [spread_block(d, block, index) for block, index in zip(blocks, maps)]
            return join(d, dot(jnp.concatenate(left, axis=1), hot))

        def layer_terms(s, w, ref, n):
            maps = [w["spot"][m] for m in range(3)]
            return slot_terms(s, maps, [ref[n, m] * w["stiff"][m] for m in range(3)], s["slot_hot"][2 * slots :, :])

        def send_layer(n, field):
            put(b["layer_send"], n, pick(d, field, v["spot"][0], lane < layer_fill[...]))
            layer_copy(n, source).start()

        early = names[:3] if site else names[:2]
        for name in early:
            load[name].wait()

        def slot_rows(w, near, far):
            return [row(w["recv"], near), row(w["recv"], far)] + ([w["spot"][m] for m in range(3)] if site else [])

        fill_nodes(d, own, v["nodes"], slot_rows(v, cross_side, mate_side))
        for name in first:
            if name in load and name not in early:
                load[name].wait()

        @pl.when(jnp.logical_not(has_cross))
        def _():
            for name in names:
                gv[name][...] = jnp.zeros_like(gv[name])
            own["w_recv"][...] = jnp.zeros_like(own["w_recv"])
            if site:
                b["layer_far"][...] = jnp.zeros_like(b["layer_far"])

        def meet_and_share():
            others = 0 if site else 1 + count(has_cross)
            pl.semaphore_wait(barrier, count(has_cross) + count(has_mate) + count(has_behind) + others)

            @pl.when(has_cross)
            def _():
                for k in range(len(names)):
                    share_copy(k).start()

        if site:
            meet_and_share()
        fill_tables(d, own, v["table"], b["square"])
        fill_matrix(d, own, v["coefs"])
        fill_state(
            d,
            [
                (own["u"], lambda c, cut: v["disp"][c, :, cut]),
                (own["prev"], lambda c, cut: v["disp"][c, :, cut] - v["vel"][c, :, cut]),
                (own["minv"], lambda c, cut: v["minv"][0, :, cut]),
            ],
        )
        near_live = lane < limit(v["fill"], cross_side)
        mate_live = lane < limit(v["fill"], mate_side)

        def ghost_setup():
            @pl.when(has_cross)
            def _():
                for k in range(len(names)):
                    share_copy(k).wait_recv()

            fill_nodes(d, ghost, gv["nodes"], slot_rows(gv, mate_side, cross_side))
            fill_matrix(d, ghost, gv["coefs"])
            fill_state(d, [(ghost["minv"], lambda c, cut: gv["minv"][0, :, cut])])

        def body(r, carry):
            n = 2 * r
            force = own["force"][...]
            put(b["cross_send"], r, pick(d, force, row(v["send"], cross_side), near_live))

            @pl.when(has_cross)
            def _():
                cross_copy(r).start()

            put(b["mate_send"], n, pick(d, force, row(v["send"], mate_side), mate_live))

            @pl.when(has_mate)
            def _():
                mate_copy(n).start()

            @pl.when(has_behind)
            def _():
                far_copy(r, behind).start()

            now = own["u"][...]
            ahead = 2.0 * now - own["prev"][...] + own["minv"][...] * force
            own["w_send"][r] = ahead

            @pl.when(has_cross)
            def _():
                w_copy(r).start()

            pl.when(r == 0)(ghost_setup)

            extra = ghost_extra = jnp.zeros_like(force)
            if site:
                for m in range(3):
                    layer_copy(n, m).wait_recv()

                @pl.when(has_cross)
                def _():
                    for m in range(3):
                        layer_ghost(r, m).wait_recv()

                extra = layer_terms(own, v, b["layer_recv"], n)
                ghost_extra = layer_terms(ghost, gv, b["layer_far"], r)

            @pl.when(has_mate)
            def _():
                mate_copy(n).wait_recv()

            @pl.when(has_cross)
            def _():
                cross_copy(r).wait_recv()

            maps = [row(v["recv"], cross_side), row(v["recv"], mate_side)]
            hot = own["slot_hot"][0 : 2 * slots, :]
            extra = extra + slot_terms(own, maps, [b["cross_recv"][r], b["mate_recv"][n]], hot)
            middle = ahead + own["minv"][...] * extra
            own["prev"][...] = now
            own["u"][...] = middle
            if not site:
                send_layer(n, middle)

                @pl.when(has_cross)
                def _():
                    layer_ghost(r, source).start()

            force = element_forces(d, own)
            put(b["mate_send"], n + 1, pick(d, force, row(v["send"], mate_side), mate_live))

            @pl.when(has_mate)
            def _():
                mate_copy(n + 1).start()

            extra = ghost_extra

            @pl.when(has_beyond)
            def _():
                far_copy(r, beyond).wait_recv()

            @pl.when(has_cross)
            def _():
                w_copy(r).wait_recv()

            ghost_maps = [row(gv["recv"], mate_side), row(gv["recv"], cross_side)]
            hot = ghost["slot_hot"][0 : 2 * slots, :]
            extra = extra + slot_terms(ghost, ghost_maps, [b["cross_send"][r], b["far_recv"][r]], hot)
            ghost["u"][...] = own["w_recv"][r] + ghost["minv"][...] * extra
            ghost_force = element_forces(d, ghost)
            ghost_live = lane < limit(gv["fill"], mate_side)
            near = jnp.concatenate(pick(d, ghost_force, row(gv["send"], mate_side), ghost_live), axis=0)

            extra = force
            if site:
                for m in range(3):
                    layer_copy(n + 1, m).wait_recv()
                extra = extra + layer_terms(own, v, b["layer_recv"], n + 1)

            @pl.when(has_mate)
            def _():
                mate_copy(n + 1).wait_recv()

            hot = own["slot_hot"][0 : 2 * slots, :]
            extra = extra + slot_terms(own, maps, [near, b["mate_recv"][n + 1]], hot)
            later = 2.0 * middle - now + own["minv"][...] * extra
            own["prev"][...] = middle
            own["u"][...] = later
            if not site:
                send_layer(n + 1, later)

            @pl.when(r < ROUNDS - 1)
            def _():
                own["force"][...] = element_forces(d, own)

            return carry

        own["force"][...] = element_forces(d, own)
        if not site:
            meet_and_share()
        lax.fori_loop(0, ROUNDS, body, 0)
        out = site_out if site else reg_out
        for c in range(3):
            for h in range(d["h"]):
                at, size = c * hp + h, min(d["width"], d["count"] - h * d["width"])
                out[c, :, h * d["width"] : h * d["width"] + size] = own["u"][at : at + 1, 0:size]

        def drain(r, carry):
            @pl.when(has_cross)
            def _():
                cross_copy(r).wait_send()
                w_copy(r).wait_send()

            @pl.when(has_behind)
            def _():
                far_copy(r, behind).wait_send()

            for n in (2 * r, 2 * r + 1):

                @pl.when(has_mate)
                def _():
                    mate_copy(n).wait_send()

                if not site:
                    layer_copy(n, source).wait_send()

            if not site:

                @pl.when(has_cross)
                def _():
                    layer_ghost(r, source).wait_send()

            return carry

        lax.fori_loop(0, ROUNDS, drain, 0)

        @pl.when(has_cross)
        def _():
            for k in range(len(names)):
                share_copy(k).wait_send()

    @pl.when(jnp.logical_not(is_site))
    def _():
        site_out[...] = jnp.zeros_like(site_out)
        role(False)

    @pl.when(is_site)
    def _():
        reg_out[...] = jnp.zeros_like(reg_out)
        role(True)


def write_out(reg_in, site_in, reg_out, site_out, sem):
    copies = [
        pltpu.make_async_copy(src, dst, sem.at[k]) for k, (src, dst) in enumerate(((site_in, site_out), (reg_in, reg_out)))
    ]
    for copy in copies:
        copy.start()
    for copy in copies:
        copy.wait()


def solution(mesh):
    n_grp, n_sub = mesh.shape["grp"], mesh.shape["sub"]

    def shards(*args):
        args = list(args)
        for k in (0, 1, 2, 3, 4, 5, 19, 20):
            rows, length = args[k].shape[2:]
            args[k] = jnp.transpose(args[k], (0, 2, 1, 3)).reshape(rows, 1, length)
        for k in (12, 13, 14, 15):
            args[k] = args[k].reshape(args[k].shape[2:])
        args[9] = args[9].T
        for k in (6, 7):
            args[k] = args[k].reshape((9,) + args[k].shape[4:])
        rd = sizes(args[4].shape, args[6].shape, args[0].shape)
        sd = sizes(args[5].shape, args[7].shape, args[2].shape)
        slots = args[12].shape[1]
        vmem = pl.BlockSpec(memory_space=pltpu.VMEM)
        hbm = pl.BlockSpec(memory_space=pltpu.HBM)
        dma = pltpu.SemaphoreType.DMA
        block = (8, slots)
        groups = {
            "common": dict(
                square=pltpu.VMEM((LANES, LANES), F32),
                cross_send=pltpu.VMEM((ROUNDS,) + block, F32),
                cross_recv=pltpu.VMEM((ROUNDS,) + block, F32),
                mate_send=pltpu.VMEM((STEPS,) + block, F32),
                mate_recv=pltpu.VMEM((STEPS,) + block, F32),
                far_recv=pltpu.VMEM((ROUNDS,) + block, F32),
                layer_send=pltpu.VMEM((STEPS,) + block, F32),
                layer_recv=pltpu.VMEM((STEPS, 3) + block, F32),
                layer_far=pltpu.VMEM((ROUNDS, 3) + block, F32),
                load_sem=dma((len(SITE_INPUTS),)),
                cross_ss=dma((ROUNDS,)),
                cross_rs=dma((ROUNDS,)),
                w_ss=dma((ROUNDS,)),
                w_rs=dma((ROUNDS,)),
                mate_ss=dma((STEPS,)),
                mate_rs=dma((STEPS,)),
                far_ss=dma((ROUNDS,)),
                far_rs=dma((ROUNDS,)),
                layer_ss=dma((STEPS,)),
                layer_rs=dma((STEPS, 3)),
                layer_gs=dma((ROUNDS,)),
                layer_gr=dma((ROUNDS, 3)),
                share_ss=dma((len(SITE_SHARED),)),
                share_rs=dma((len(SITE_SHARED),)),
            )
        }
        for prefix, d, numbers, shared, slot_rows in (
            ("reg", rd, REG_INPUTS, REG_SHARED, 2),
            ("site", sd, SITE_INPUTS, SITE_SHARED, 5),
        ):
            places = {name: pltpu.VMEM(args[k].shape, args[k].dtype) for name, k in zip(NAMES, numbers)}
            groups[prefix + "_in"] = places
            groups[prefix + "_ghost_in"] = {name: places[name] for name in shared}
            groups[prefix + "_shared"] = role_scratch(d, slots)
            groups[prefix + "_own"] = part_scratch(d, slot_rows, slots)
            groups[prefix + "_ghost"] = part_scratch(d, slot_rows, slots)
        keys = [(group, list(items)) for group, items in groups.items()]
        reg_out, site_out = pl.pallas_call(
            functools.partial(kernel, n_grp, n_sub, rd, sd, slots, keys),
            out_shape=(
                jax.ShapeDtypeStruct(args[0].shape, F32),
                jax.ShapeDtypeStruct(args[2].shape, F32),
            ),
            in_specs=[vmem if k == SCALAR else hbm for k in range(len(args))],
            out_specs=(vmem, vmem),
            scratch_shapes=[place for items in groups.values() for place in items.values()],
            compiler_params=pltpu.CompilerParams(
                collective_id=0, has_side_effects=True, vmem_limit_bytes=32 * 1024 * 1024
            ),
        )(*[arg if k == SCALAR else pltpu.with_memory_space_constraint(arg, pltpu.HBM) for k, arg in enumerate(args)])
        outs = (reg_out, site_out)
        outs = pl.pallas_call(
            write_out,
            out_shape=tuple(jax.ShapeDtypeStruct(out.shape, F32) for out in outs),
            in_specs=[vmem] * 2,
            out_specs=(hbm, hbm),
            scratch_shapes=[dma((2,))],
            compiler_params=pltpu.CompilerParams(vmem_limit_bytes=1024 * 1024),
        )(*outs)
        return tuple(out.reshape(1, 1, out.shape[0], out.shape[2]) for out in outs)

    cell = ("grp", "sub")
    specs = [P(*cell)] * 21
    specs[8] = specs[9] = P()
    return jax.shard_map(
        shards,
        mesh=mesh,
        in_specs=tuple(specs),
        out_specs=(P(*cell), P(*cell)),
        check_vma=False,
    )
```

```python
import functools

import jax
import jax.numpy as jnp
from jax import lax
from jax.experimental import pallas as pl
from jax.experimental.pallas import tpu as pltpu
from jax.sharding import PartitionSpec as P

STEPS = 8
ROUNDS = STEPS // 2
LANES = 128
MESH = pl.DeviceIdType.MESH
F32 = jnp.float32
BF16 = jnp.bfloat16


def up(size, unit):
    return -(-size // unit) * unit


def lane_gather(block, index):
    numbers = lax.GatherDimensionNumbers(
        offset_dims=(),
        collapsed_slice_dims=(1,),
        start_index_map=(1,),
        operand_batching_dims=(0,),
        start_indices_batching_dims=(0,),
    )
    return lax.gather(
        block,
        index[..., None],
        numbers,
        slice_sizes=(1, 1),
        mode=lax.GatherScatterMode.PROMISE_IN_BOUNDS,
    )


def split(value):
    high = value.astype(BF16)
    low = (value - high.astype(F32)).astype(BF16)
    return high, low


def dot(left, right):
    return jnp.dot(left, right, preferred_element_type=F32)


def sizes(nodes_shape, coefs_shape, disp_shape):
    p, _, e = nodes_shape
    q = coefs_shape[-2]
    count = disp_shape[-1]
    width = LANES
    h = -(-count // width)
    qp = up(q, 8)
    return dict(
        p=p, e=e, q=q, count=count, width=width, shift=width.bit_length() - 1, h=h, hp=h, rows=up(3 * h, 8), qp=qp,
        p8=up(p, 8), kw=up(9 * qp, LANES),
    )


def part_scratch(d, slot_rows, slots):
    state = (d["rows"], d["width"])
    return dict(
        lane=pltpu.VMEM((d["p8"], d["e"]), jnp.int32),
        block=pltpu.VMEM((d["p8"], d["e"]), jnp.int32),
        hot=pltpu.VMEM((d["p"] * d["e"], d["width"]), BF16),
        slot_hot=pltpu.VMEM((slot_rows * slots, d["width"]), BF16),
        fe=pltpu.VMEM((2, d["p8"], 3 * d["e"]), F32),
        ve=pltpu.VMEM((3, d["p8"], d["e"]), F32),
        matrix=pltpu.VMEM((d["p"] * d["p8"], d["e"]), F32),
        u=pltpu.VMEM(state, F32),
        minv=pltpu.VMEM(state, F32),
    )


def role_scratch(d, slots):
    state = (d["rows"], d["width"])
    return dict(
        wide=pltpu.VMEM((2, d["p8"], d["kw"]), F32),
        weight=pltpu.VMEM((2, up(d["p"] * d["p8"], 16), d["kw"]), BF16),
        cube=pltpu.VMEM((9 * d["qp"], d["e"]), F32),
        turn=pltpu.VMEM((LANES, max(d["e"], slots)), F32),
        prev=pltpu.VMEM(state, F32),
        force=pltpu.VMEM(state, F32),
        w_send=pltpu.VMEM((ROUNDS,) + state, F32),
        w_recv=pltpu.VMEM((ROUNDS,) + state, F32),
    )


def fill_onehot(d, out_ref, rows, turn):
    length = rows[0].shape[1]
    for r, row in enumerate(rows):
        turn[r : r + 1, 0:length] = (row & (d["width"] - 1)).astype(F32)
    columns = turn[:, 0:length].T.astype(BF16)
    lane = lax.broadcasted_iota(jnp.int32, (length, d["width"]), 1).astype(F32).astype(BF16)
    one, zero = jnp.ones((), BF16), jnp.zeros((), BF16)
    for r in range(len(rows)):
        hot = jnp.where(lane == columns[:, r : r + 1], one, zero)
        out_ref[r * length : (r + 1) * length, :] = hot


def fill_tables(d, s, table, square):
    p, q, qp, p8 = d["p"], d["q"], d["qp"], d["p8"]
    wide = s["wide"]
    wide[...] = jnp.zeros_like(wide)
    if table.shape[0] != p:
        square[...] = jnp.zeros_like(square)
        square[0 : 3 * q, 0:p] = table[...]
        square[...] = square[...].T
        table = square
    for a in range(3):
        for b in range(3):
            at = (3 * a + b) * qp
            wide[0, 0:p, at : at + q] = table[0:p, a * q : (a + 1) * q]
            wide[1, 0:p, at : at + q] = table[0:p, b * q : (b + 1) * q]
    left = -wide[0]
    for first in range(0, p, 2):
        rows = range(first, min(p, first + 2))
        high, low = split(jnp.concatenate([left * wide[1, n : n + 1, :] for n in rows], axis=0))
        cut = slice(first * p8, (rows[-1] + 1) * p8)
        s["weight"][0, cut, :] = high
        s["weight"][1, cut, :] = low


def fill_nodes(d, s, nodes, slot_rows):
    p = d["p"]
    s["lane"][...] = jnp.zeros_like(s["lane"])
    s["block"][...] = jnp.full_like(s["block"], -1)
    for r in range(p):
        s["lane"][r : r + 1, :] = nodes[r] & (LANES - 1)
        s["block"][r : r + 1, :] = nodes[r] >> 7
    s["turn"][...] = jnp.zeros_like(s["turn"])
    fill_onehot(d, s["hot"], [nodes[r] for r in range(p)], s["turn"])
    fill_onehot(d, s["slot_hot"], slot_rows, s["turn"])


def fill_state(d, pairs):
    hp, width, count = d["hp"], d["width"], d["count"]
    for ref, _ in pairs:
        ref[...] = jnp.zeros_like(ref)
    for c in range(3):
        for h in range(d["h"]):
            size = min(width, count - h * width)
            at, cut = c * hp + h, slice(h * width, h * width + size)
            for ref, value in pairs:
                ref[at : at + 1, 0:size] = value(c, cut)


def fill_matrix(d, s, coefs):
    q, qp, p, p8, e, depth = d["q"], d["qp"], d["p"], d["p8"], d["e"], 9 * d["qp"]
    if qp != q:
        s["cube"][...] = jnp.zeros_like(s["cube"])
    for k in range(9):
        s["cube"][k * qp : k * qp + q, :] = coefs[k]
    high, low = split(s["cube"][...])
    both = jnp.concatenate([high, low], axis=1)
    for first in range(0, p, 2):
        cut = slice(first * p8, min(p, first + 2) * p8)
        wide = dot(s["weight"][0, cut, 0:depth], both)
        s["matrix"][cut, :] = wide[:, 0:e] + wide[:, e:] + dot(s["weight"][1, cut, 0:depth], high)


def spread(d, rows, blocks):
    lanes, hp = rows[0].shape[1], d["hp"]
    place = lax.broadcasted_iota(jnp.int32, (8, lanes), 0)
    out = []
    for k in range(len(rows) // 3):
        for first in range(0, d["rows"], 8):
            value, wanted = None, None
            for c in range(3):
                low, high = c * hp - first, (c + 1) * hp - first
                if high <= 0 or low >= 8:
                    continue
                row, block = jnp.broadcast_to(rows[3 * k + c], (8, lanes)), place - low
                value = row if value is None else jnp.where(place < low, value, row)
                wanted = block if wanted is None else jnp.where(place < low, wanted, block)
            if first + 8 > 3 * hp:
                wanted = jnp.where(place < 3 * hp - first, wanted, -2)
            out.append(jnp.where(wanted == blocks, value, 0.0))
    return jnp.concatenate(out, axis=0).astype(BF16)


def spread_block(d, block, index):
    high = block.astype(BF16).astype(F32)
    low = block - high
    rows = [part[c : c + 1] for part in (high, low) for c in range(3)]
    return spread(d, rows, index >> d["shift"])


def join(d, total):
    half = d["rows"]
    return total[0:half] + total[half:]


def pick(d, field, index, live):
    count, slots = d["rows"], index.shape[1]
    got = lane_gather(field, jnp.broadcast_to(index & (LANES - 1), (count, slots)))
    blocks = jnp.where(live, index >> d["shift"], -4 * count)
    place = lax.broadcasted_iota(jnp.int32, (count, slots), 0)
    return [
        jnp.sum(jnp.where(place == blocks + c * d["hp"], got, 0.0), axis=0, keepdims=True) for c in range(3)
    ]


def element_forces(d, s):
    p, e, p8, hp = d["p"], d["e"], d["p8"], d["hp"]
    parts = d["width"] // LANES
    blocks128 = -(-d["count"] // LANES)
    groups = p8 // 8
    for t in range(e // LANES):
        cut = slice(t * LANES, (t + 1) * LANES)
        for g in range(groups):
            lane = s["lane"][8 * g : 8 * g + 8, cut]
            block = s["block"][8 * g : 8 * g + 8, cut]
            bits = [(block >> k) & 1 == 1 for k in range((blocks128 - 1).bit_length())]
            for c in range(3):
                values = []
                for h in range(blocks128):
                    at, part = h // parts, h % parts
                    row = s["u"][c * hp + at : c * hp + at + 1, part * LANES : (part + 1) * LANES]
                    values.append(lane_gather(jnp.broadcast_to(row, (8, LANES)), lane))
                for bit in bits:
                    values = [
                        jnp.where(bit, values[k + 1], values[k]) if k + 1 < len(values) else values[k]
                        for k in range(0, len(values), 2)
                    ]
                s["ve"][c, 8 * g : 8 * g + 8, cut] = values[0]
        total = [[None] * groups for _ in range(3)]
        for n in range(p):
            rows = [s["ve"][c, n : n + 1, cut] for c in range(3)]
            for g in range(groups):
                weight = s["matrix"][n * p8 + 8 * g : n * p8 + 8 * g + 8, cut]
                for c in range(3):
                    term = weight * rows[c]
                    total[c][g] = term if n == 0 else total[c][g] + term
        for g in range(groups):
            for c in range(3):
                high = total[c][g].astype(BF16).astype(F32)
                at = slice(c * e + t * LANES, c * e + (t + 1) * LANES)
                s["fe"][0, 8 * g : 8 * g + 8, at] = high
                s["fe"][1, 8 * g : 8 * g + 8, at] = total[c][g] - high
    up_shift = parts.bit_length() - 1
    step = max(1, 2 * LANES // e)
    total = None
    for first in range(0, p, step):
        chunk = range(first, min(p, first + step))
        left = []
        for n in chunk:
            rows = [s["fe"][k, n : n + 1, c * e : (c + 1) * e] for k in range(2) for c in range(3)]
            left.append(spread(d, rows, s["block"][n : n + 1, :] >> up_shift))
        piece = dot(jnp.concatenate(left, axis=1), s["hot"][first * e : (chunk[-1] + 1) * e, :])
        total = piece if total is None else total + piece
    return join(d, total)


SCALAR = 18
REG_INPUTS = (0, 1, 4, 6, 8, 10, 12, 13, 16, 17)
SITE_INPUTS = (2, 3, 5, 7, 9, 11, 14, 15, 16, 19, 20)
NAMES = ("disp", "vel", "nodes", "coefs", "table", "minv", "send", "recv", "fill", "spot", "stiff")
REG_SHARED = ("nodes", "recv", "send", "fill", "minv", "coefs")
SITE_SHARED = ("nodes", "recv", "spot", "send", "fill", "minv", "stiff", "coefs")


def kernel(n_grp, n_sub, rd, sd, slots, keys, *refs):
    inputs, (reg_out, site_out), refs = refs[:21], refs[21:23], refs[23:]
    layer_fill = inputs[SCALAR]
    box = {}
    for group, names in keys:
        box[group], refs = dict(zip(names, refs)), refs[len(names) :]
    b = box["common"]
    sites = n_grp // 4
    regs = 3 * sites
    grp, sub = lax.axis_index("grp"), lax.axis_index("sub")
    is_site = grp >= regs
    source, part = grp // sites, grp % sites
    odd = lax.rem(sub, 2)
    cross_side, mate_side = odd, 1 - odd
    way = 2 * odd - 1
    cross, mate, beyond, behind = sub + way, sub - way, sub + 2 * way, sub - 2 * way

    def exists(place):
        return jnp.logical_and(place >= 0, place < n_sub)

    has_cross, has_mate, has_beyond, has_behind = (exists(place) for place in (cross, mate, beyond, behind))

    def count(flag):
        return jnp.where(flag, 1, 0)

    def remote(src, dst, send_sem, recv_sem, target):
        return pltpu.make_async_remote_copy(
            src_ref=src, dst_ref=dst, send_sem=send_sem, recv_sem=recv_sem, device_id=target, device_id_type=MESH
        )

    def loads(numbers, places):
        return {
            name: pltpu.make_async_copy(inputs[k], places[name], b["load_sem"].at[i])
            for i, (name, k) in enumerate(zip(NAMES, numbers))
        }

    reg_loads, site_loads = loads(REG_INPUTS, box["reg_in"]), loads(SITE_INPUTS, box["site_in"])
    first = ("nodes", "recv", "spot", "table", "coefs", "disp", "vel", "minv", "send", "fill", "stiff")

    @pl.when(jnp.logical_not(is_site))
    def _():
        for name in first:
            if name in reg_loads:
                reg_loads[name].start()

    @pl.when(is_site)
    def _():
        for name in first:
            site_loads[name].start()

    barrier = pltpu.get_barrier_semaphore()

    def greet(target):
        pl.semaphore_signal(barrier, inc=1, device_id=target, device_id_type=MESH)

    for flag, place in ((has_cross, cross), (has_mate, mate), (has_beyond, beyond)):

        @pl.when(flag)
        def _():
            greet((grp, place))

    @pl.when(is_site)
    def _():
        for m in range(3):
            greet((m * sites + part, sub))

    @pl.when(jnp.logical_and(is_site, has_cross))
    def _():
        for m in range(3):
            greet((m * sites + part, cross))

    for name in ("cross_send", "mate_send", "layer_send"):
        b[name][...] = jnp.zeros_like(b[name])

    for flag, names in ((has_cross, ("cross_recv",)), (has_mate, ("mate_recv",)), (has_beyond, ("far_recv",))):

        @pl.when(jnp.logical_not(flag))
        def _():
            for name in names:
                b[name][...] = jnp.zeros_like(b[name])

    lane = lax.broadcasted_iota(jnp.int32, (1, slots), 1)

    def role(site):
        prefix = "site" if site else "reg"
        d = sd if site else rd
        v, gv = box[prefix + "_in"], box[prefix + "_ghost_in"]
        shared, own, ghost = box[prefix + "_shared"], dict(box[prefix + "_own"]), dict(box[prefix + "_ghost"])
        for s in (own, ghost):
            s.update(shared)
        load = site_loads if site else reg_loads
        names = SITE_SHARED if site else REG_SHARED
        first_fill = 2 if site else 0
        hp = d["hp"]

        def cross_copy(r):
            return remote(b["cross_send"].at[r], b["cross_recv"].at[r], b["cross_ss"].at[r], b["cross_rs"].at[r], (grp, cross))

        def w_copy(r):
            return remote(own["w_send"].at[r], own["w_recv"].at[r], b["w_ss"].at[r], b["w_rs"].at[r], (grp, cross))

        def mate_copy(n):
            return remote(b["mate_send"].at[n], b["mate_recv"].at[n], b["mate_ss"].at[n], b["mate_rs"].at[n], (grp, mate))

        def far_copy(r, target):
            return remote(b["mate_send"].at[2 * r], b["far_recv"].at[r], b["far_ss"].at[r], b["far_rs"].at[r], (grp, target))

        def share_copy(k):
            return remote(v[names[k]], gv[names[k]], b["share_ss"].at[k], b["share_rs"].at[k], (grp, cross))

        def layer_copy(n, m):
            return remote(
                b["layer_send"].at[n], b["layer_recv"].at[n, m], b["layer_ss"].at[n], b["layer_rs"].at[n, m],
                (regs + part, sub),
            )

        def layer_ghost(r, m):
            return remote(
                b["layer_send"].at[2 * r], b["layer_far"].at[r, m], b["layer_gs"].at[r], b["layer_gr"].at[r, m],
                (regs + part, cross),
            )

        def limit(fills, side):
            low, high = (fills[0, :, first_fill + k : first_fill + k + 1] for k in range(2))
            return jnp.where(side == 0, low, high)

        def row(ref, side):
            return ref[pl.ds(side, 1), :]

        def put(ref, n, rows):
            for c in range(3):
                ref[n, c : c + 1, :] = rows[c]

        def slot_terms(s, maps, blocks, hot):
            left = [spread_block(d, block, index) for block, index in zip(blocks, maps)]
            return join(d, dot(jnp.concatenate(left, axis=1), hot))

        def layer_terms(s, w, ref, n):
            maps = [w["spot"][m] for m in range(3)]
            return slot_terms(s, maps, [ref[n, m] * w["stiff"][m] for m in range(3)], s["slot_hot"][2 * slots :, :])

        def send_layer(n, field):
            put(b["layer_send"], n, pick(d, field, v["spot"][0], lane < layer_fill[...]))
            layer_copy(n, source).start()

        early = names[:3] if site else names[:2]
        for name in early:
            load[name].wait()

        def slot_rows(w, near, far):
            return [row(w["recv"], near), row(w["recv"], far)] + ([w["spot"][m] for m in range(3)] if site else [])

        fill_nodes(d, own, v["nodes"], slot_rows(v, cross_side, mate_side))
        for name in first:
            if name in load and name not in early:
                load[name].wait()

        @pl.when(jnp.logical_not(has_cross))
        def _():
            for name in names:
                gv[name][...] = jnp.zeros_like(gv[name])
            own["w_recv"][...] = jnp.zeros_like(own["w_recv"])
            if site:
                b["layer_far"][...] = jnp.zeros_like(b["layer_far"])

        def meet_and_share():
            others = 0 if site else 1 + count(has_cross)
            pl.semaphore_wait(barrier, count(has_cross) + count(has_mate) + count(has_behind) + others)

            @pl.when(has_cross)
            def _():
                for k in range(len(names)):
                    share_copy(k).start()

        if site:
            meet_and_share()
        fill_tables(d, own, v["table"], b["square"])
        fill_matrix(d, own, v["coefs"])
        fill_state(
            d,
            [
                (own["u"], lambda c, cut: v["disp"][c, :, cut]),
                (own["prev"], lambda c, cut: v["disp"][c, :, cut] - v["vel"][c, :, cut]),
                (own["minv"], lambda c, cut: v["minv"][0, :, cut]),
            ],
        )
        near_live = lane < limit(v["fill"], cross_side)
        mate_live = lane < limit(v["fill"], mate_side)

        def ghost_setup():
            @pl.when(has_cross)
            def _():
                for k in range(len(names)):
                    share_copy(k).wait_recv()

            fill_nodes(d, ghost, gv["nodes"], slot_rows(gv, mate_side, cross_side))
            fill_matrix(d, ghost, gv["coefs"])
            fill_state(d, [(ghost["minv"], lambda c, cut: gv["minv"][0, :, cut])])

        def body(r, carry):
            n = 2 * r
            force = own["force"][...]
            put(b["cross_send"], r, pick(d, force, row(v["send"], cross_side), near_live))

            @pl.when(has_cross)
            def _():
                cross_copy(r).start()

            put(b["mate_send"], n, pick(d, force, row(v["send"], mate_side), mate_live))

            @pl.when(has_mate)
            def _():
                mate_copy(n).start()

            @pl.when(has_behind)
            def _():
                far_copy(r, behind).start()

            now = own["u"][...]
            ahead = 2.0 * now - own["prev"][...] + own["minv"][...] * force
            own["w_send"][r] = ahead

            @pl.when(has_cross)
            def _():
                w_copy(r).start()

            pl.when(r == 0)(ghost_setup)

            extra = ghost_extra = jnp.zeros_like(force)
            if site:
                for m in range(3):
                    layer_copy(n, m).wait_recv()

                @pl.when(has_cross)
                def _():
                    for m in range(3):
                        layer_ghost(r, m).wait_recv()

                extra = layer_terms(own, v, b["layer_recv"], n)
                ghost_extra = layer_terms(ghost, gv, b["layer_far"], r)

            @pl.when(has_mate)
            def _():
                mate_copy(n).wait_recv()

            @pl.when(has_cross)
            def _():
                cross_copy(r).wait_recv()

            maps = [row(v["recv"], cross_side), row(v["recv"], mate_side)]
            hot = own["slot_hot"][0 : 2 * slots, :]
            extra = extra + slot_terms(own, maps, [b["cross_recv"][r], b["mate_recv"][n]], hot)
            middle = ahead + own["minv"][...] * extra
            own["prev"][...] = now
            own["u"][...] = middle
            if not site:
                send_layer(n, middle)

                @pl.when(has_cross)
                def _():
                    layer_ghost(r, source).start()

            force = element_forces(d, own)
            put(b["mate_send"], n + 1, pick(d, force, row(v["send"], mate_side), mate_live))

            @pl.when(has_mate)
            def _():
                mate_copy(n + 1).start()

            extra = ghost_extra

            @pl.when(has_beyond)
            def _():
                far_copy(r, beyond).wait_recv()

            @pl.when(has_cross)
            def _():
                w_copy(r).wait_recv()

            ghost_maps = [row(gv["recv"], mate_side), row(gv["recv"], cross_side)]
            hot = ghost["slot_hot"][0 : 2 * slots, :]
            extra = extra + slot_terms(ghost, ghost_maps, [b["cross_send"][r], b["far_recv"][r]], hot)
            ghost["u"][...] = own["w_recv"][r] + ghost["minv"][...] * extra
            ghost_force = element_forces(d, ghost)
            ghost_live = lane < limit(gv["fill"], mate_side)
            near = jnp.concatenate(pick(d, ghost_force, row(gv["send"], mate_side), ghost_live), axis=0)

            extra = force
            if site:
                for m in range(3):
                    layer_copy(n + 1, m).wait_recv()
                extra = extra + layer_terms(own, v, b["layer_recv"], n + 1)

            @pl.when(has_mate)
            def _():
                mate_copy(n + 1).wait_recv()

            hot = own["slot_hot"][0 : 2 * slots, :]
            extra = extra + slot_terms(own, maps, [near, b["mate_recv"][n + 1]], hot)
            later = 2.0 * middle - now + own["minv"][...] * extra
            own["prev"][...] = middle
            own["u"][...] = later
            if not site:
                send_layer(n + 1, later)

            @pl.when(r < ROUNDS - 1)
            def _():
                own["force"][...] = element_forces(d, own)

            return carry

        own["force"][...] = element_forces(d, own)
        if not site:
            meet_and_share()
        lax.fori_loop(0, ROUNDS, body, 0)
        out = site_out if site else reg_out
        for c in range(3):
            for h in range(d["h"]):
                at, size = c * hp + h, min(d["width"], d["count"] - h * d["width"])
                out[c, :, h * d["width"] : h * d["width"] + size] = own["u"][at : at + 1, 0:size]

        def drain(r, carry):
            @pl.when(has_cross)
            def _():
                cross_copy(r).wait_send()
                w_copy(r).wait_send()

            @pl.when(has_behind)
            def _():
                far_copy(r, behind).wait_send()

            for n in (2 * r, 2 * r + 1):

                @pl.when(has_mate)
                def _():
                    mate_copy(n).wait_send()

                if not site:
                    layer_copy(n, source).wait_send()

            if not site:

                @pl.when(has_cross)
                def _():
                    layer_ghost(r, source).wait_send()

            return carry

        lax.fori_loop(0, ROUNDS, drain, 0)

        @pl.when(has_cross)
        def _():
            for k in range(len(names)):
                share_copy(k).wait_send()

    @pl.when(jnp.logical_not(is_site))
    def _():
        site_out[...] = jnp.zeros_like(site_out)
        role(False)

    @pl.when(is_site)
    def _():
        reg_out[...] = jnp.zeros_like(reg_out)
        role(True)


def write_out(reg_in, site_in, reg_out, site_out, sem):
    copies = [
        pltpu.make_async_copy(src, dst, sem.at[k]) for k, (src, dst) in enumerate(((site_in, site_out), (reg_in, reg_out)))
    ]
    for copy in copies:
        copy.start()
    for copy in copies:
        copy.wait()


def solution(mesh):
    n_grp, n_sub = mesh.shape["grp"], mesh.shape["sub"]

    def shards(*args):
        args = list(args)
        for k in (0, 1, 2, 3, 4, 5, 19, 20):
            rows, length = args[k].shape[2:]
            args[k] = jnp.transpose(args[k], (0, 2, 1, 3)).reshape(rows, 1, length)
        for k in (12, 13, 14, 15):
            args[k] = args[k].reshape(args[k].shape[2:])
        args[9] = args[9].T
        for k in (6, 7):
            args[k] = args[k].reshape((9,) + args[k].shape[4:])
        rd = sizes(args[4].shape, args[6].shape, args[0].shape)
        sd = sizes(args[5].shape, args[7].shape, args[2].shape)
        slots = args[12].shape[1]
        vmem = pl.BlockSpec(memory_space=pltpu.VMEM)
        hbm = pl.BlockSpec(memory_space=pltpu.HBM)
        dma = pltpu.SemaphoreType.DMA
        block = (8, slots)
        groups = {
            "common": dict(
                square=pltpu.VMEM((LANES, LANES), F32),
                cross_send=pltpu.VMEM((ROUNDS,) + block, F32),
                cross_recv=pltpu.VMEM((ROUNDS,) + block, F32),
                mate_send=pltpu.VMEM((STEPS,) + block, F32),
                mate_recv=pltpu.VMEM((STEPS,) + block, F32),
                far_recv=pltpu.VMEM((ROUNDS,) + block, F32),
                layer_send=pltpu.VMEM((STEPS,) + block, F32),
                layer_recv=pltpu.VMEM((STEPS, 3) + block, F32),
                layer_far=pltpu.VMEM((ROUNDS, 3) + block, F32),
                load_sem=dma((len(SITE_INPUTS),)),
                cross_ss=dma((ROUNDS,)),
                cross_rs=dma((ROUNDS,)),
                w_ss=dma((ROUNDS,)),
                w_rs=dma((ROUNDS,)),
                mate_ss=dma((STEPS,)),
                mate_rs=dma((STEPS,)),
                far_ss=dma((ROUNDS,)),
                far_rs=dma((ROUNDS,)),
                layer_ss=dma((STEPS,)),
                layer_rs=dma((STEPS, 3)),
                layer_gs=dma((ROUNDS,)),
                layer_gr=dma((ROUNDS, 3)),
                share_ss=dma((len(SITE_SHARED),)),
                share_rs=dma((len(SITE_SHARED),)),
            )
        }
        for prefix, d, numbers, shared, slot_rows in (
            ("reg", rd, REG_INPUTS, REG_SHARED, 2),
            ("site", sd, SITE_INPUTS, SITE_SHARED, 5),
        ):
            places = {name: pltpu.VMEM(args[k].shape, args[k].dtype) for name, k in zip(NAMES, numbers)}
            groups[prefix + "_in"] = places
            groups[prefix + "_ghost_in"] = {name: places[name] for name in shared}
            groups[prefix + "_shared"] = role_scratch(d, slots)
            groups[prefix + "_own"] = part_scratch(d, slot_rows, slots)
            groups[prefix + "_ghost"] = part_scratch(d, slot_rows, slots)
        keys = [(group, list(items)) for group, items in groups.items()]
        reg_out, site_out = pl.pallas_call(
            functools.partial(kernel, n_grp, n_sub, rd, sd, slots, keys),
            out_shape=(
                jax.ShapeDtypeStruct(args[0].shape, F32),
                jax.ShapeDtypeStruct(args[2].shape, F32),
            ),
            in_specs=[vmem if k == SCALAR else hbm for k in range(len(args))],
            out_specs=(vmem, vmem),
            scratch_shapes=[place for items in groups.values() for place in items.values()],
            compiler_params=pltpu.CompilerParams(
                collective_id=0, has_side_effects=True, vmem_limit_bytes=32 * 1024 * 1024
            ),
        )(*[arg if k == SCALAR else pltpu.with_memory_space_constraint(arg, pltpu.HBM) for k, arg in enumerate(args)])
        outs = (reg_out, site_out)
        outs = pl.pallas_call(
            write_out,
            out_shape=tuple(jax.ShapeDtypeStruct(out.shape, F32) for out in outs),
            in_specs=[vmem] * 2,
            out_specs=(hbm, hbm),
            scratch_shapes=[dma((2,))],
            compiler_params=pltpu.CompilerParams(vmem_limit_bytes=1024 * 1024),
        )(*outs)
        return tuple(out.reshape(1, 1, out.shape[0], out.shape[2]) for out in outs)

    cell = ("grp", "sub")
    specs = [P(*cell)] * 21
    specs[8] = specs[9] = P()
    return jax.shard_map(
        shards,
        mesh=mesh,
        in_specs=tuple(specs),
        out_specs=(P(*cell), P(*cell)),
        check_vma=False,
    )
```
